32 devices in a mesh: dp: 2 (over x), ep: 16 (over z, y, core).
Axes of the slice: x: 2, y: 2, z: 4, core: 2. Of those that a mesh axis runs over, the one named last changes fastest.
Arguments:
- hidden_in: bfloat16 [1024, 2048], P(('dp', 'ep')), parts along dimension 0
- kv_cache: bfloat16 [1024, 256, 576], P(('dp', 'ep')), parts along dimension 0
- kv_lens: int32 [1024], P(('dp', 'ep')), parts along dimension 0
- routes: int32 [1024, 6], P(('dp', 'ep')), parts along dimension 0
- route_gates: float32 [1024, 6], P(('dp', 'ep')), parts along dimension 0
- w_q: bfloat16 [2048, 3072], replicated
- w_dkv: bfloat16 [2048, 576], replicated
- w_uk: bfloat16 [16, 128, 512], replicated
- w_uv: bfloat16 [16, 512, 128], replicated
- w_o: bfloat16 [2048, 2048], replicated
- sh_gate: bfloat16 [2048, 2816], replicated
- sh_up: bfloat16 [2048, 2816], replicated
- sh_down: bfloat16 [2816, 2048], replicated
- ex_gate: bfloat16 [64, 2048, 1408], P('ep')
- ex_up: bfloat16 [64, 2048, 1408], P('ep')
- ex_down: bfloat16 [64, 1408, 2048], P('ep')
Outputs:
- output 1: bfloat16 [1024, 2048], P(('dp', 'ep')), parts along dimension 0
- output 2: bfloat16 [1024, 576], P(('dp', 'ep')), parts along dimension 0
There are 2 independent parts. The reference program is written for one: setup_inputs(seed, part) draws one part's arguments, and reference() takes and returns one part's arrays. A program takes and returns all parts, laid end to end along the dimension named above; an argument that names none is the same for every part.
All inputs are finite; a program needn't handle non-finite values.
Results may differ from the reference program's by a relative error of at most 0.0158526.
Values are sent between devices in bfloat16 or wider.
A program may use at most 1 GiB of HBM per device.

```python
import jax
import jax.numpy as jnp
from jax import lax

HIDDEN = 2048
NUM_HEADS = 16
NOPE_DIM = 128
ROPE_DIM = 64
V_DIM = 128
LATENT = 512
EXPERTS = 64
TOP_K = 6
MOE_FF = 1408
SHARED_FF = 2816
SEQS_DEV = 32
CACHE_LEN = 256
GROUP_SIZE = 16


def draw_lengths(rng_key):
    key_dev, key_seq, key_top = jax.random.split(rng_key, 3)
    key_shift, key_mant = jax.random.split(key_dev)
    num_seq = GROUP_SIZE * SEQS_DEV
    dev_shift = jax.random.randint(key_shift, (GROUP_SIZE, 1), 1, 5, jnp.int32)
    dev_mant = jax.random.randint(key_mant, (GROUP_SIZE, 1), 0, 256, jnp.int32)
    dev_num = (256 + dev_mant) >> dev_shift
    seq_draw = jax.random.randint(key_seq, (GROUP_SIZE, SEQS_DEV), 0, CACHE_LEN, jnp.int32)
    lengths = ((dev_num * seq_draw) >> 8).astype(jnp.int32).reshape(num_seq)
    lengths = jnp.minimum(lengths, CACHE_LEN - 1)
    top_pos = jax.random.randint(key_top, (), 0, num_seq)
    return jnp.where(jnp.arange(num_seq) == top_pos, CACHE_LEN - 1, lengths).astype(jnp.int32)


def draw_routes(rng_key):
    n_hot = GROUP_SIZE // 4
    n_cold = GROUP_SIZE - n_hot
    hot_picks = (3 * TOP_K) // 4
    local_exp = EXPERTS // GROUP_SIZE
    key_perm, key_hot, key_cold, key_exp, key_order = jax.random.split(rng_key, 5)
    dev_order = jax.random.permutation(key_perm, GROUP_SIZE)
    exp_shift = jax.random.randint(key_exp, (GROUP_SIZE, GROUP_SIZE), 0, local_exp)
    src_dev = jnp.arange(GROUP_SIZE)[:, None]

    def pick_experts(dev_list, dev_count, per_token, shift_key):
        pos_shift = jax.random.randint(shift_key, (GROUP_SIZE, 1), 0, dev_count)
        copy_pos = jnp.arange(SEQS_DEV * per_token)[None, :] + pos_shift
        dst_dev = dev_list[copy_pos % dev_count]
        local_id = (copy_pos // dev_count + exp_shift[src_dev, dst_dev]) % local_exp
        return (dst_dev * local_exp + local_id).reshape(GROUP_SIZE, SEQS_DEV, per_token)

    hot_ids = pick_experts(dev_order[:n_hot], n_hot, hot_picks, key_hot)
    cold_ids = pick_experts(dev_order[n_hot:], n_cold, TOP_K - hot_picks, key_cold)
    all_ids = jnp.concatenate([hot_ids, cold_ids], axis=2).reshape(GROUP_SIZE * SEQS_DEV, TOP_K)
    col_order = jnp.argsort(jax.random.uniform(key_order, (GROUP_SIZE * SEQS_DEV, TOP_K), jnp.float32), axis=1)
    return jnp.take_along_axis(all_ids, col_order, axis=1).astype(jnp.int32)


def setup_inputs(seed: int = 0, part: int = 0) -> dict:
    base_key = jax.random.key(seed)
    part_keys = jax.random.split(jax.random.fold_in(base_key, part), 5)
    weight_keys = jax.random.split(base_key, 11)
    num_seq = GROUP_SIZE * SEQS_DEV
    lat_row = LATENT + ROPE_DIM

    def normal_w(rng_key, shape_w, fan_in, gain_mul):
        return (jax.random.normal(rng_key, shape_w, jnp.float32) * (gain_mul * fan_in ** -0.5)).astype(jnp.bfloat16)

    return {
        "hidden_in": jax.random.normal(part_keys[0], (num_seq, HIDDEN), jnp.float32).astype(jnp.bfloat16),
        "kv_cache": jax.random.normal(part_keys[1], (num_seq, CACHE_LEN, lat_row), jnp.float32).astype(jnp.bfloat16),
        "kv_lens": draw_lengths(part_keys[2]),
        "routes": draw_routes(part_keys[3]),
        "route_gates": jax.nn.softmax(0.7 * jax.random.normal(part_keys[4], (num_seq, TOP_K), jnp.float32), axis=-1),
        "w_q": normal_w(weight_keys[0], (HIDDEN, NUM_HEADS * (NOPE_DIM + ROPE_DIM)), HIDDEN, 1.0),
        "w_dkv": normal_w(weight_keys[1], (HIDDEN, lat_row), HIDDEN, 1.0),
        "w_uk": normal_w(weight_keys[2], (NUM_HEADS, NOPE_DIM, LATENT), NOPE_DIM, 1.0),
        "w_uv": normal_w(weight_keys[3], (NUM_HEADS, LATENT, V_DIM), LATENT, 3.0),
        "w_o": normal_w(weight_keys[4], (NUM_HEADS * V_DIM, HIDDEN), NUM_HEADS * V_DIM, 1.0),
        "sh_gate": normal_w(weight_keys[5], (HIDDEN, SHARED_FF), HIDDEN, 1.0),
        "sh_up": normal_w(weight_keys[6], (HIDDEN, SHARED_FF), HIDDEN, 1.0),
        "sh_down": normal_w(weight_keys[7], (SHARED_FF, HIDDEN), SHARED_FF, 1.0),
        "ex_gate": normal_w(weight_keys[8], (EXPERTS, HIDDEN, MOE_FF), HIDDEN, 1.0),
        "ex_up": normal_w(weight_keys[9], (EXPERTS, HIDDEN, MOE_FF), HIDDEN, 1.0),
        "ex_down": normal_w(weight_keys[10], (EXPERTS, MOE_FF, HIDDEN), MOE_FF, 1.0),
    }


def rotary(vec, cos_t, sin_t):
    half_dim = vec.shape[-1] // 2
    lead_part = vec[..., :half_dim]
    tail_part = vec[..., half_dim:]
    return jnp.concatenate([lead_part * cos_t - tail_part * sin_t, tail_part * cos_t + lead_part * sin_t], axis=-1)


def rotary_table(positions, rot_width):
    half_dim = rot_width // 2
    inv_freq = jnp.exp(jnp.arange(half_dim, dtype=jnp.float32) * (-2.0 * jnp.log(10000.0) / rot_width))
    angle_val = positions.astype(jnp.float32)[:, None] * inv_freq[None, :]
    return jnp.cos(angle_val), jnp.sin(angle_val)


def swiglu(rows_in, w_gate, w_up, w_down):
    gate_val = jnp.dot(rows_in, w_gate, preferred_element_type=jnp.float32)
    up_val = jnp.dot(rows_in, w_up, preferred_element_type=jnp.float32)
    act_val = (jax.nn.silu(gate_val) * up_val).astype(jnp.bfloat16)
    return jnp.dot(act_val, w_down, preferred_element_type=jnp.float32).astype(jnp.bfloat16)


def attend_block(x_blk, cache_blk, len_blk, w_q, w_dkv, w_uk, w_uv, w_o):
    num_seq = x_blk.shape[0]
    q_all = jnp.dot(x_blk, w_q, preferred_element_type=jnp.float32).astype(jnp.bfloat16)
    q_all = q_all.reshape(num_seq, NUM_HEADS, NOPE_DIM + ROPE_DIM)
    kv_raw = jnp.dot(x_blk, w_dkv, preferred_element_type=jnp.float32)
    cos_t, sin_t = rotary_table(len_blk, ROPE_DIM)
    kv_row = jnp.concatenate([kv_raw[:, :LATENT], rotary(kv_raw[:, LATENT:], cos_t, sin_t)], axis=1).astype(jnp.bfloat16)
    q_rope = rotary(q_all[:, :, NOPE_DIM:].astype(jnp.float32), cos_t[:, None, :], sin_t[:, None, :]).astype(jnp.bfloat16)
    q_lat = jnp.einsum("bhn,hnc->bhc", q_all[:, :, :NOPE_DIM].astype(jnp.float32), w_uk.astype(jnp.float32)).astype(jnp.bfloat16)
    q_cat = jnp.concatenate([q_lat, q_rope], axis=2).astype(jnp.float32)
    score_scale = (NOPE_DIM + ROPE_DIM) ** -0.5
    cache_wide = cache_blk.astype(jnp.float32)
    kv_wide = kv_row.astype(jnp.float32)
    s_old = jnp.einsum("bhc,blc->bhl", q_cat, cache_wide) * score_scale
    s_new = jnp.einsum("bhc,bc->bh", q_cat, kv_wide) * score_scale
    valid_mask = jnp.arange(CACHE_LEN)[None, None, :] < len_blk[:, None, None]
    s_old = jnp.where(valid_mask, s_old, -jnp.inf)
    top_score = jnp.maximum(jnp.max(s_old, axis=2), s_new)
    e_old = jnp.exp(s_old - top_score[:, :, None])
    e_new = jnp.exp(s_new - top_score)
    denom_sum = jnp.sum(e_old, axis=2) + e_new
    p_old = (e_old / denom_sum[:, :, None]).astype(jnp.bfloat16).astype(jnp.float32)
    p_new = (e_new / denom_sum).astype(jnp.bfloat16).astype(jnp.float32)
    o_full = jnp.einsum("bhl,blc->bhc", p_old, cache_wide) + p_new[:, :, None] * kv_wide[:, None, :]
    o_lat = o_full[:, :, :LATENT].astype(jnp.bfloat16)
    v_head = jnp.einsum("bhc,hcv->bhv", o_lat.astype(jnp.float32), w_uv.astype(jnp.float32)).astype(jnp.bfloat16)
    attn_out = jnp.dot(v_head.reshape(num_seq, NUM_HEADS * V_DIM), w_o, preferred_element_type=jnp.float32).astype(jnp.bfloat16)
    h_mid = (x_blk.astype(jnp.float32) + attn_out.astype(jnp.float32)).astype(jnp.bfloat16)
    return h_mid, kv_row


def reference(hidden_in, kv_cache, kv_lens, routes, route_gates, w_q, w_dkv, w_uk, w_uv, w_o, sh_gate, sh_up, sh_down, ex_gate, ex_up, ex_down):
    num_seq = GROUP_SIZE * SEQS_DEV
    lat_row = LATENT + ROPE_DIM

    def per_device(dev_blocks):
        return attend_block(dev_blocks[0], dev_blocks[1], dev_blocks[2], w_q, w_dkv, w_uk, w_uv, w_o)

    h_mid, kv_row = lax.map(per_device, (hidden_in.reshape(GROUP_SIZE, SEQS_DEV, HIDDEN), kv_cache.reshape(GROUP_SIZE, SEQS_DEV, CACHE_LEN, lat_row), kv_lens.reshape(GROUP_SIZE, SEQS_DEV)))
    h_mid = h_mid.reshape(num_seq, HIDDEN)
    kv_row = kv_row.reshape(num_seq, lat_row)
    shared = swiglu(h_mid, sh_gate, sh_up, sh_down)
    local_exp = EXPERTS // GROUP_SIZE
    hot_devs = GROUP_SIZE // 4
    pair_cap = (SEQS_DEV * ((3 * TOP_K) // 4) + hot_devs - 1) // hot_devs
    exp_cap = (pair_cap + local_exp - 1) // local_exp
    rows_per_exp = GROUP_SIZE * exp_cap
    ids_dev = routes.reshape(GROUP_SIZE, SEQS_DEV * TOP_K)
    onehot = (ids_dev[:, :, None] == jnp.arange(EXPERTS)[None, None, :]).astype(jnp.int32)
    rank_pos = jnp.sum((jnp.cumsum(onehot, axis=1) - onehot) * onehot, axis=2)
    row_pos = (ids_dev * rows_per_exp + jnp.arange(GROUP_SIZE)[:, None] * exp_cap + rank_pos).reshape(-1)
    token_ids = jnp.arange(num_seq * TOP_K) // TOP_K
    table_tok = jnp.zeros((EXPERTS * rows_per_exp,), jnp.int32).at[row_pos].set(token_ids)
    table_gate = jnp.zeros((EXPERTS * rows_per_exp,), jnp.float32).at[row_pos].set(route_gates.reshape(-1))

    def add_expert(routed_acc, per_exp):
        exp_tok = per_exp[3]
        exp_out = swiglu(jnp.take(h_mid, exp_tok, axis=0), per_exp[0], per_exp[1], per_exp[2])
        routed_acc = routed_acc + jax.ops.segment_sum(exp_out.astype(jnp.float32) * per_exp[4][:, None], exp_tok, num_segments=num_seq)
        return routed_acc, None

    routed = lax.scan(add_expert, jnp.zeros((num_seq, HIDDEN), jnp.float32), (ex_gate, ex_up, ex_down, table_tok.reshape(EXPERTS, rows_per_exp), table_gate.reshape(EXPERTS, rows_per_exp)))[0]
    layer_out = (h_mid.astype(jnp.float32) + shared.astype(jnp.float32) + routed).astype(jnp.bfloat16)
    return (layer_out, kv_row)
```

```python
import jax
import jax.numpy as jnp
from jax import lax
from jax.sharding import PartitionSpec as P


def rotary(vec, cos_t, sin_t):
    half_dim = vec.shape[-1] // 2
    lead_part = vec[..., :half_dim]
    tail_part = vec[..., half_dim:]
    return jnp.concatenate([lead_part * cos_t - tail_part * sin_t, tail_part * cos_t + lead_part * sin_t], axis=-1)


def rotary_table(positions, rot_width):
    half_dim = rot_width // 2
    inv_freq = jnp.exp(jnp.arange(half_dim, dtype=jnp.float32) * (-2.0 * jnp.log(10000.0) / rot_width))
    angle_val = positions.astype(jnp.float32)[:, None] * inv_freq[None, :]
    return jnp.cos(angle_val), jnp.sin(angle_val)


def attend_local(x_blk, cache_blk, len_blk, w_q, w_dkv, w_uk, w_uv, w_o):
    num_seq = x_blk.shape[0]
    num_heads, nope_dim, latent = w_uk.shape
    rope_dim = cache_blk.shape[2] - latent
    v_dim = w_uv.shape[2]
    q_all = jnp.dot(x_blk, w_q, preferred_element_type=jnp.float32).astype(jnp.bfloat16).reshape(num_seq, num_heads, nope_dim + rope_dim)
    kv_raw = jnp.dot(x_blk, w_dkv, preferred_element_type=jnp.float32)
    cos_t, sin_t = rotary_table(len_blk, rope_dim)
    kv_row = jnp.concatenate([kv_raw[:, :latent], rotary(kv_raw[:, latent:], cos_t, sin_t)], axis=1).astype(jnp.bfloat16)
    q_rope = rotary(q_all[:, :, nope_dim:].astype(jnp.float32), cos_t[:, None, :], sin_t[:, None, :]).astype(jnp.bfloat16)
    q_lat = jnp.einsum("bhn,hnc->bhc", q_all[:, :, :nope_dim], w_uk, preferred_element_type=jnp.float32).astype(jnp.bfloat16)
    q_cat = jnp.concatenate([q_lat, q_rope], axis=2)
    score_scale = (nope_dim + rope_dim) ** -0.5
    s_old = jnp.einsum("bhc,blc->bhl", q_cat, cache_blk, preferred_element_type=jnp.float32) * score_scale
    s_new = jnp.einsum("bhc,bc->bh", q_cat, kv_row, preferred_element_type=jnp.float32) * score_scale
    valid_mask = jnp.arange(cache_blk.shape[1])[None, None, :] < len_blk[:, None, None]
    s_old = jnp.where(valid_mask, s_old, -jnp.inf)
    top_score = jnp.maximum(jnp.max(s_old, axis=2), s_new)
    e_old = jnp.exp(s_old - top_score[:, :, None])
    e_new = jnp.exp(s_new - top_score)
    denom_sum = jnp.sum(e_old, axis=2) + e_new
    p_old = (e_old / denom_sum[:, :, None]).astype(jnp.bfloat16)
    p_new = (e_new / denom_sum).astype(jnp.bfloat16)
    o_full = jnp.einsum("bhl,blc->bhc", p_old, cache_blk, preferred_element_type=jnp.float32) + p_new.astype(jnp.float32)[:, :, None] * kv_row.astype(jnp.float32)[:, None, :]
    o_lat = o_full[:, :, :latent].astype(jnp.bfloat16)
    v_head = jnp.einsum("bhc,hcv->bhv", o_lat, w_uv, preferred_element_type=jnp.float32).astype(jnp.bfloat16)
    attn_out = jnp.dot(v_head.reshape(num_seq, num_heads * v_dim), w_o, preferred_element_type=jnp.float32).astype(jnp.bfloat16)
    h_mid = (x_blk.astype(jnp.float32) + attn_out.astype(jnp.float32)).astype(jnp.bfloat16)
    return h_mid, kv_row


def swiglu(rows_in, w_gate, w_up, w_down):
    gate_val = jnp.dot(rows_in, w_gate, preferred_element_type=jnp.float32)
    up_val = jnp.dot(rows_in, w_up, preferred_element_type=jnp.float32)
    act_val = (jax.nn.silu(gate_val) * up_val).astype(jnp.bfloat16)
    return jnp.dot(act_val, w_down, preferred_element_type=jnp.float32).astype(jnp.bfloat16)


def expert_rows(row_buf, ex_gate, ex_up, ex_down):
    gate_val = jnp.einsum("gch,ghf->gcf", row_buf, ex_gate, preferred_element_type=jnp.float32)
    up_val = jnp.einsum("gch,ghf->gcf", row_buf, ex_up, preferred_element_type=jnp.float32)
    act_val = (jax.nn.silu(gate_val) * up_val).astype(jnp.bfloat16)
    return jnp.einsum("gcf,gfh->gch", act_val, ex_down, preferred_element_type=jnp.float32).astype(jnp.bfloat16)


def expert_cap(seqs_dev, top_k, group_size, local_exp):
    hot_devs = group_size // 4
    pair_cap = (seqs_dev * ((3 * top_k) // 4) + hot_devs - 1) // hot_devs
    return (pair_cap + local_exp - 1) // local_exp


def solution(mesh):
    group_size = mesh.shape["ep"]

    def device_step(x_blk, cache_blk, len_blk, routes, route_gates, w_q, w_dkv, w_uk, w_uv, w_o, sh_gate, sh_up, sh_down, ex_gate, ex_up, ex_down):
        num_seq, hidden = x_blk.shape
        top_k = routes.shape[1]
        local_exp = ex_gate.shape[0]
        exp_cap = expert_cap(num_seq, top_k, group_size, local_exp)
        h_mid, kv_row = attend_local(x_blk, cache_blk, len_blk, w_q, w_dkv, w_uk, w_uv, w_o)
        shared = swiglu(h_mid, sh_gate, sh_up, sh_down)
        me = lax.axis_index("ep")
        ids_all = lax.all_gather(routes, "ep", tiled=True)
        gates_all = lax.all_gather(route_gates, "ep", tiled=True)
        h_all = lax.all_gather(h_mid, "ep", tiled=True)
        num_tok = num_seq * group_size
        exp_ids = me * local_exp + jnp.arange(local_exp, dtype=jnp.int32)
        hit = ids_all[:, :, None] == exp_ids[None, None, :]
        member = jnp.any(hit, axis=1)
        gate_te = jnp.sum(jnp.where(hit, gates_all[:, :, None], 0.0), axis=1)
        tri = (jnp.arange(num_seq)[:, None] > jnp.arange(num_seq)[None, :]).astype(jnp.bfloat16)
        rank = jnp.einsum("ts,dse->dte", tri, member.astype(jnp.bfloat16).reshape(group_size, num_seq, local_exp), preferred_element_type=jnp.float32)
        base = (jnp.arange(group_size, dtype=jnp.int32) * exp_cap)[:, None, None]
        slot = jnp.where(member, (rank.astype(jnp.int32) + base).reshape(num_tok, local_exp), -1)
        rows_exp = group_size * exp_cap
        pick = (slot.T[:, None, :] == jnp.arange(rows_exp, dtype=jnp.int32)[None, :, None]).astype(jnp.bfloat16)
        recv = jnp.einsum("est,th->esh", pick, h_all, preferred_element_type=jnp.float32).astype(jnp.bfloat16)
        exp_out = expert_rows(recv, ex_gate, ex_up, ex_down)
        back = jnp.einsum("est,esh->eth", pick, exp_out, preferred_element_type=jnp.float32)
        part = jnp.sum(back * gate_te.T[:, :, None], axis=0)
        routed = lax.psum_scatter(part, "ep", scatter_dimension=0, tiled=True)
        layer_out = (h_mid.astype(jnp.float32) + shared.astype(jnp.float32) + routed).astype(jnp.bfloat16)
        return layer_out, kv_row

    batch_spec = P(("dp", "ep"))
    weight_spec = P()
    expert_spec = P("ep")
    in_specs = (batch_spec,) * 5 + (weight_spec,) * 8 + (expert_spec,) * 3
    return jax.shard_map(device_step, mesh=mesh, in_specs=in_specs, out_specs=(batch_spec, batch_spec), check_vma=False)
```

```python
import functools

import jax
import jax.numpy as jnp
from jax import lax
from jax.experimental import pallas as pl
from jax.experimental.pallas import tpu as pltpu
from jax.sharding import PartitionSpec as P

MESH = pl.DeviceIdType.MESH
BF = jnp.bfloat16
F32 = jnp.float32


def rotary(vec, cos_t, sin_t):
    half_dim = vec.shape[-1] // 2
    lead_part = vec[..., :half_dim]
    tail_part = vec[..., half_dim:]
    return jnp.concatenate([lead_part * cos_t - tail_part * sin_t, tail_part * cos_t + lead_part * sin_t], axis=-1)


def rotary_table(positions, rot_width):
    half_dim = rot_width // 2
    inv_freq = jnp.exp(jnp.arange(half_dim, dtype=jnp.float32) * (-2.0 * jnp.log(10000.0) / rot_width))
    angle_val = positions.astype(jnp.float32)[:, None] * inv_freq[None, :]
    return jnp.cos(angle_val), jnp.sin(angle_val)


def attend_local(x_blk, cache_blk, len_blk, w_q, w_dkv, w_uk, w_uv, w_o):
    num_seq = x_blk.shape[0]
    num_heads, nope_dim, latent = w_uk.shape
    rope_dim = cache_blk.shape[2] - latent
    v_dim = w_uv.shape[2]
    q_all = jnp.dot(x_blk, w_q, preferred_element_type=jnp.float32).astype(jnp.bfloat16).reshape(num_seq, num_heads, nope_dim + rope_dim)
    kv_raw = jnp.dot(x_blk, w_dkv, preferred_element_type=jnp.float32)
    cos_t, sin_t = rotary_table(len_blk, rope_dim)
    kv_row = jnp.concatenate([kv_raw[:, :latent], rotary(kv_raw[:, latent:], cos_t, sin_t)], axis=1).astype(jnp.bfloat16)
    q_rope = rotary(q_all[:, :, nope_dim:].astype(jnp.float32), cos_t[:, None, :], sin_t[:, None, :]).astype(jnp.bfloat16)
    q_lat = jnp.einsum("bhn,hnc->bhc", q_all[:, :, :nope_dim], w_uk, preferred_element_type=jnp.float32).astype(jnp.bfloat16)
    q_cat = jnp.concatenate([q_lat, q_rope], axis=2)
    score_scale = (nope_dim + rope_dim) ** -0.5
    s_old = jnp.einsum("bhc,blc->bhl", q_cat, cache_blk, preferred_element_type=jnp.float32) * score_scale
    s_new = jnp.einsum("bhc,bc->bh", q_cat, kv_row, preferred_element_type=jnp.float32) * score_scale
    valid_mask = jnp.arange(cache_blk.shape[1])[None, None, :] < len_blk[:, None, None]
    s_old = jnp.where(valid_mask, s_old, -jnp.inf)
    top_score = jnp.maximum(jnp.max(s_old, axis=2), s_new)
    e_old = jnp.exp(s_old - top_score[:, :, None])
    e_new = jnp.exp(s_new - top_score)
    denom_sum = jnp.sum(e_old, axis=2) + e_new
    p_old = (e_old / denom_sum[:, :, None]).astype(jnp.bfloat16)
    p_new = (e_new / denom_sum).astype(jnp.bfloat16)
    o_full = jnp.einsum("bhl,blc->bhc", p_old, cache_blk, preferred_element_type=jnp.float32) + p_new.astype(jnp.float32)[:, :, None] * kv_row.astype(jnp.float32)[:, None, :]
    o_lat = o_full[:, :, :latent].astype(jnp.bfloat16)
    v_head = jnp.einsum("bhc,hcv->bhv", o_lat, w_uv, preferred_element_type=jnp.float32).astype(jnp.bfloat16)
    attn_out = jnp.dot(v_head.reshape(num_seq, num_heads * v_dim), w_o, preferred_element_type=jnp.float32).astype(jnp.bfloat16)
    h_mid = (x_blk.astype(jnp.float32) + attn_out.astype(jnp.float32)).astype(jnp.bfloat16)
    return h_mid, kv_row


def route_meta(routes, route_gates, num_exp):
    hit = routes[:, :, None] == jnp.arange(num_exp, dtype=jnp.int32)[None, None, :]
    member = jnp.any(hit, axis=1)
    gate_te = jnp.sum(jnp.where(hit, route_gates[:, :, None], 0.0), axis=1)
    num_seq = routes.shape[0]
    tri = (jnp.arange(num_seq)[:, None] > jnp.arange(num_seq)[None, :]).astype(BF)
    rank = jnp.dot(tri, member.astype(BF), preferred_element_type=F32)
    return jnp.concatenate([jnp.where(member, rank, -4096.0), gate_te], axis=1)


NG = 5
ND = 8
NCH = 4


def moe_kernel(h_ref, meta_ref, sg_ref, su_ref, sd_ref, eg_ref, eu_ref, ed_ref, out_ref,
               gbuf, dbuf, h_all, meta_all, meta_t, sel, sel_t, gates, xe, act, act_sh, shared,
               part, rc, ry, rz,
               gsem, dsem, ag_send, ag_recv, am_send, am_recv,
               s1_send, s1_recv, s2_send, s2_recv, s3_send, s3_recv):
    me = lax.axis_index("ep")
    c = lax.rem(me, 2)
    y = lax.rem(lax.div(me, 2), 2)
    z = lax.div(me, 4)
    core_peer = me + 1 - 2 * c
    y_peer = me + 2 - 4 * y
    zs = [lax.rem(z + d, 4) for d in range(4)]
    zback = [lax.rem(z + 4 - d, 4) for d in range(4)]
    z_peers = [me + 4 * (zs[d] - z) for d in range(4)]
    num_loc, hidden, ff = eg_ref.shape
    num_seq = h_ref.shape[0]
    cw = hidden // NCH

    def g_copy(k):
        slot = k % NG
        if k < 4:
            src = (sg_ref, su_ref)[k % 2].at[:, pl.ds((k // 2) * ff, ff)]
        else:
            src = (eg_ref, eu_ref)[k % 2].at[(k - 4) // 2]
        return pltpu.make_async_copy(src, gbuf.at[slot], gsem.at[slot])

    def d_copy(p):
        slot = p % ND
        if p < 8:
            src = sd_ref.at[pl.ds((p % 2) * ff, ff), pl.ds((p // 2) * cw, cw)]
        else:
            q = p - 8
            src = ed_ref.at[q % 4, :, pl.ds((q // 4) * cw, cw)]
        return pltpu.make_async_copy(src, dbuf.at[slot], dsem.at[slot])

    for k in range(4):
        g_copy(k).start()
    for p in range(ND):
        d_copy(p).start()
    g_copy(4).start()

    barrier = pltpu.get_barrier_semaphore()
    peers = [core_peer, y_peer, z_peers[1], z_peers[2], z_peers[3]]
    for peer in peers:
        pl.semaphore_signal(barrier, inc=1, device_id={"ep": peer}, device_id_type=MESH)
    pl.semaphore_wait(barrier, len(peers))

    def ag(src_pos, peer, n, own=False):
        cc, yy, zz = src_pos
        idx = (cc * 2 + yy) * 4 + zz
        hb = h_ref if own else h_all.at[cc, yy, zz]
        mb = meta_ref if own else meta_all.at[cc, yy, zz]
        a = pltpu.make_async_remote_copy(src_ref=mb, dst_ref=meta_all.at[cc, yy, zz], send_sem=am_send.at[n], recv_sem=am_recv.at[idx], device_id={"ep": peer}, device_id_type=MESH)
        b = pltpu.make_async_remote_copy(src_ref=hb, dst_ref=h_all.at[cc, yy, zz], send_sem=ag_send.at[n], recv_sem=ag_recv.at[idx], device_id={"ep": peer}, device_id_type=MESH)
        return a, b

    started = []

    def send(src_pos, peer, n, own=False):
        a, b = ag(src_pos, peer, n, own)
        a.start()
        b.start()
        started.append((a, b))

    def arrive(src_pos):
        a, b = ag(src_pos, core_peer, 0)
        a.wait_recv()
        b.wait_recv()

    mine = (c, y, z)
    send(mine, y_peer, 0, True)
    for d in (1, 2, 3):
        send(mine, z_peers[d], d, True)
    send(mine, core_peer, 4, True)
    h_all[c, y, z] = h_ref[...]
    meta_all[c, y, z] = meta_ref[...]

    def fwd_z(d):
        pos = (c, y, zback[d])
        arrive(pos)
        send(pos, y_peer, 4 + d)
        send(pos, core_peer, 7 + d)

    def fwd_y(d):
        pos = (c, 1 - y, zback[d])
        arrive(pos)
        send(pos, core_peer, 11 + d)

    def gate_up(x, gslot, uslot, store):
        def block(start, size):
            g = jnp.dot(x(), gbuf[gslot, :, pl.ds(start, size)], preferred_element_type=F32)
            u = jnp.dot(x(), gbuf[uslot, :, pl.ds(start, size)], preferred_element_type=F32)
            store(start, size, (g * jax.nn.sigmoid(g) * u).astype(BF))

        @pl.loop(0, ff // 256)
        def _(n):
            block(pl.multiple_of(n * 256, 256), 256)

        if ff % 256:
            block(ff - ff % 256, ff % 256)

    def g_wait(k):
        g_copy(k).wait()

    for s in range(2):
        g_wait(2 * s)
        g_wait(2 * s + 1)

        def put(start, size, v, s=s):
            act_sh[s, :, pl.ds(start, size)] = v
        gate_up(lambda: h_ref[...], (2 * s) % NG, (2 * s + 1) % NG, put)
        g_copy(2 * s + 5).start()
        g_copy(2 * s + 6).start()
        if s == 0:
            fwd_z(1)
            fwd_y(0)
        else:
            fwd_z(2)
            fwd_z(3)
    for j in range(NCH):
        d_copy(2 * j).wait()
        d_copy(2 * j + 1).wait()
        o = jnp.dot(act_sh[0], dbuf[2 * j], preferred_element_type=F32) + jnp.dot(act_sh[1], dbuf[2 * j + 1], preferred_element_type=F32)
        shared[:, j * cw:(j + 1) * cw] = o.astype(BF)
        d_copy(2 * j + 8).start()
        d_copy(2 * j + 9).start()
        if j >= 1:
            fwd_y(j)
    for yy in range(2):
        for zz in range(4):
            arrive((1 - c, yy, zz))

    ntok = 16 * num_seq
    rows = 16 * 8
    meta = meta_all[...].reshape(ntok, 128)
    meta_t[...] = meta.T
    lane = lax.broadcasted_iota(jnp.int32, (ntok, 128), 1)
    base_col = lax.broadcasted_iota(jnp.int32, (ntok, 128), 0) // num_seq * 8
    base_row = lax.broadcasted_iota(jnp.int32, (1, ntok), 1) // num_seq * 8
    slot_row = lax.broadcasted_iota(jnp.int32, (rows, ntok), 0)
    for e in range(num_loc):
        ge = me * num_loc + e
        code = jnp.sum(jnp.where(lane == ge, meta, 0.0), axis=1, keepdims=True)
        gate = jnp.sum(jnp.where(lane == ge + 64, meta, 0.0), axis=1, keepdims=True)
        sel[e] = jnp.where(lane == code.astype(jnp.int32) + base_col, 1.0, 0.0).astype(BF)
        gates[e] = jnp.broadcast_to(gate, (ntok, 128))
        code_t = meta_t[pl.ds(ge, 1), :].astype(jnp.int32) + base_row
        sel_t[pl.ds(e * rows, rows), :] = jnp.where(slot_row == code_t, 1.0, 0.0).astype(BF)

    @pl.loop(0, hidden // 512)
    def _(n):
        cols = pl.ds(pl.multiple_of(n * 512, 512), 512)
        hh = h_all[:, :, :, :, cols].reshape(ntok, 512)
        xe[:, cols] = jnp.dot(sel_t[...], hh, preferred_element_type=F32).astype(BF)

    for e in range(num_loc):
        g_wait(4 + 2 * e)
        g_wait(5 + 2 * e)

        def put(start, size, v, e=e):
            act[e, :, pl.ds(start, size)] = v
        gate_up(lambda e=e: xe[pl.ds(e * rows, rows), :], (4 + 2 * e) % NG, (5 + 2 * e) % NG, put)
        for k in (9 + 2 * e, 10 + 2 * e):
            if k < 4 + 2 * num_loc:
                g_copy(k).start()

    def s1(j):
        cols = pl.ds(j * cw, cw)
        return pltpu.make_async_remote_copy(src_ref=part.at[1 - c, :, :, :, cols], dst_ref=rc.at[:, :, :, cols], send_sem=s1_send.at[j], recv_sem=s1_recv.at[j], device_id={"ep": core_peer}, device_id_type=MESH)

    def s2(j):
        cols = pl.ds(j * cw, cw)
        return pltpu.make_async_remote_copy(src_ref=part.at[c, 1 - y, :, :, cols], dst_ref=ry.at[:, :, cols], send_sem=s2_send.at[j], recv_sem=s2_recv.at[j], device_id={"ep": y_peer}, device_id_type=MESH)

    def s3(j, d):
        cols = pl.ds(j * cw, cw)
        return pltpu.make_async_remote_copy(src_ref=part.at[c, y, zs[d], :, cols], dst_ref=rz.at[d - 1, :, cols], send_sem=s3_send.at[j * 3 + d - 1], recv_sem=s3_recv.at[j * 3 + d - 1], device_id={"ep": z_peers[d]}, device_id_type=MESH)

    def after_s1(j):
        cols = slice(j * cw, (j + 1) * cw)
        s1(j).wait_recv()
        part[c, 1 - y, :, :, cols] = part[c, 1 - y, :, :, cols] + rc[1 - y, :, :, cols]
        s2(j).start()
        part[c, y, :, :, cols] = part[c, y, :, :, cols] + rc[y, :, :, cols]

    def after_s2(j):
        cols = slice(j * cw, (j + 1) * cw)
        s2(j).wait_recv()
        part[c, y, :, :, cols] = part[c, y, :, :, cols] + ry[:, :, cols]
        for d in (2, 1, 3):
            s3(j, d).start()

    def down(j):
        cols = pl.ds(j * cw, cw)
        for e in range(num_loc):
            p = 8 + 4 * j + e
            d_copy(p).wait()
        for e in range(num_loc):
            p = 8 + 4 * j + e
            o = jnp.dot(act[e], dbuf[p % ND], preferred_element_type=F32).astype(BF)
            if p + ND < 8 + 4 * NCH:
                d_copy(p + ND).start()
            for g in range(4):
                tok = pl.ds(g * ntok // 4, ntok // 4)
                b = jnp.dot(sel[e, tok, :], o, preferred_element_type=F32)
                gt = gates[e, tok, :]
                b = b * jnp.concatenate([gt] * (cw // 128), axis=1)
                b = b.reshape(4, num_seq, cw)
                if e == 0:
                    part[g // 2, g % 2, :, :, cols] = b
                else:
                    part[g // 2, g % 2, :, :, cols] = part[g // 2, g % 2, :, :, cols] + b

    for j in range(NCH):
        down(j)
        s1(j).start()
        if j >= 1:
            after_s1(j - 1)
        if j >= 2:
            after_s2(j - 2)
    after_s1(NCH - 1)
    after_s2(NCH - 2)
    after_s2(NCH - 1)
    for j in range(NCH):
        cols = slice(j * cw, (j + 1) * cw)
        for d in (1, 2, 3):
            s3(j, d).wait_recv()
        routed = part[c, y, z, :, cols] + rz[0, :, cols] + rz[1, :, cols] + rz[2, :, cols]
        out_ref[:, cols] = (h_ref[:, cols].astype(F32) + shared[:, cols].astype(F32) + routed).astype(BF)
    for a, b in started:
        a.wait_send()
        b.wait_send()
    for j in range(NCH):
        s1(j).wait_send()
        s2(j).wait_send()
        for d in (1, 2, 3):
            s3(j, d).wait_send()


def moe(h, meta, sh_gate, sh_up, sh_down, ex_gate, ex_up, ex_down):
    num_seq, hidden = h.shape
    num_loc, _, ff = ex_gate.shape
    ntok = 16 * num_seq
    dma = pltpu.SemaphoreType.DMA
    vm = pl.BlockSpec(memory_space=pltpu.VMEM)
    hbm = pl.BlockSpec(memory_space=pl.ANY)
    return pl.pallas_call(
        moe_kernel,
        out_shape=jax.ShapeDtypeStruct((num_seq, hidden), BF),
        in_specs=[vm, vm] + [hbm] * 6,
        out_specs=vm,
        scratch_shapes=[
            pltpu.VMEM((NG, hidden, ff), BF),
            pltpu.VMEM((ND, ff, hidden // NCH), BF),
            pltpu.VMEM((2, 2, 4, num_seq, hidden), BF),
            pltpu.VMEM((2, 2, 4, num_seq, 128), F32),
            pltpu.VMEM((128, ntok), F32),
            pltpu.VMEM((num_loc, ntok, 128), BF),
            pltpu.VMEM((num_loc * 128, ntok), BF),
            pltpu.VMEM((num_loc, ntok, 128), F32),
            pltpu.VMEM((num_loc * 128, hidden), BF),
            pltpu.VMEM((num_loc, 128, ff), BF),
            pltpu.VMEM((2, num_seq, ff), BF),
            pltpu.VMEM((num_seq, hidden), BF),
            pltpu.VMEM((2, 2, 4, num_seq, hidden), F32),
            pltpu.VMEM((2, 4, num_seq, hidden), F32),
            pltpu.VMEM((4, num_seq, hidden), F32),
            pltpu.VMEM((3, num_seq, hidden), F32),
            dma((NG,)), dma((ND,)), dma((15,)), dma((16,)), dma((15,)), dma((16,)),
            dma((NCH,)), dma((NCH,)), dma((NCH,)), dma((NCH,)), dma((3 * NCH,)), dma((3 * NCH,)),
        ],
        compiler_params=pltpu.CompilerParams(collective_id=0, has_side_effects=True, vmem_limit_bytes=67043328),
        name="moe",
    )(h, meta, sh_gate, sh_up, sh_down, ex_gate, ex_up, ex_down)


def solution(mesh):
    group_size = mesh.shape["ep"]

    def device_step(x_blk, cache_blk, len_blk, routes, route_gates, w_q, w_dkv, w_uk, w_uv, w_o, sh_gate, sh_up, sh_down, ex_gate, ex_up, ex_down):
        num_exp = ex_gate.shape[0] * group_size
        meta = route_meta(routes, route_gates, num_exp)
        h_mid, kv_row = attend_local(x_blk, cache_blk, len_blk, w_q, w_dkv, w_uk, w_uv, w_o)
        layer_out = moe(h_mid, meta, sh_gate, sh_up, sh_down, ex_gate, ex_up, ex_down)
        return layer_out, kv_row

    batch_spec = P(("dp", "ep"))
    weight_spec = P()
    expert_spec = P("ep")
    in_specs = (batch_spec,) * 5 + (weight_spec,) * 8 + (expert_spec,) * 3
    return jax.shard_map(device_step, mesh=mesh, in_specs=in_specs, out_specs=(batch_spec, batch_spec), check_vma=False)
```

```python
import functools

import jax
import jax.numpy as jnp
from jax import lax
from jax.experimental import pallas as pl
from jax.experimental.pallas import tpu as pltpu
from jax.sharding import PartitionSpec as P

MESH = pl.DeviceIdType.MESH
BF = jnp.bfloat16
F32 = jnp.float32


NG = 5
ND = 8
NCH = 4


def layer_kernel(x_ref, len_ref, routes_ref, rgate_ref, cache_ref, wq_ref, wdkv_ref, wuk_ref, wuv_ref, wo_ref,
                 sg_ref, su_ref, sd_ref, eg_ref, eu_ref, ed_ref, out_ref, kv_ref,
                 gbuf, dbuf, cbuf, dkv_buf, qn, kvf, vcat, h_own, meta_own,
                 h_all, meta_all, meta_t, sel, sel_t, gates, xe, act, act_sh, shared,
                 part, rc, ry, rz,
                 gsem, dsem, csem, xsem, ag_send, ag_recv, am_send, am_recv,
                 s1_send, s1_recv, s2_send, s2_recv, s3_send, s3_recv):
    me = lax.axis_index("ep")
    c = lax.rem(me, 2)
    y = lax.rem(lax.div(me, 2), 2)
    z = lax.div(me, 4)
    core_peer = me + 1 - 2 * c
    y_peer = me + 2 - 4 * y
    zs = [lax.rem(z + d, 4) for d in range(4)]
    zback = [lax.rem(z + 4 - d, 4) for d in range(4)]
    z_peers = [me + 4 * (zs[d] - z) for d in range(4)]
    num_loc, hidden, ff = eg_ref.shape
    num_seq = x_ref.shape[0]
    cw = hidden // NCH
    latent = wuk_ref.shape[1]
    num_heads = part.shape[0] * part.shape[1] * part.shape[2]
    nope = wuk_ref.shape[0] // num_heads
    rope = wdkv_ref.shape[1] - latent
    qw = nope + rope
    top_k = routes_ref.shape[1]

    W6 = 6 * qw
    W4 = 4 * qw
    OB = hidden - ff

    def g_copy(k):
        slot = k % NG
        dst = gbuf.at[slot]
        if k < 2:
            src, dst = wq_ref.at[:, pl.ds(k * W6, W6)], gbuf.at[slot, :, pl.ds(0, W6)]
        elif k == 2:
            src, dst = wq_ref.at[:, pl.ds(2 * W6, W4)], gbuf.at[slot, :, pl.ds(0, W4)]
        elif k == 3:
            src, dst = wo_ref.at[:, pl.ds(ff, OB)], gbuf.at[slot, :, pl.ds(0, OB)]
        elif k == 4:
            src = wo_ref.at[:, pl.ds(0, ff)]
        elif k < 9:
            src = (su_ref, sg_ref)[k % 2].at[:, pl.ds((k - 5) // 2 * ff, ff)]
        else:
            src = (eu_ref, eg_ref)[k % 2].at[(k - 9) // 2]
        return pltpu.make_async_copy(src, dst, gsem.at[slot])

    def uk_copy():
        return pltpu.make_async_copy(wuk_ref, gbuf.at[2, :, pl.ds(W4, latent)], xsem.at[0])

    def uv_copy(i):
        return pltpu.make_async_copy(wuv_ref.at[pl.ds(i * hidden, hidden)], gbuf.at[3, :, pl.ds(OB + 128 * i, 128)], xsem.at[1 + i])

    def dkv_copy():
        return pltpu.make_async_copy(wdkv_ref, dkv_buf, xsem.at[5])

    def c_copy(g, slot):
        return pltpu.make_async_copy(cache_ref.at[pl.ds(g * 8, 8)], cbuf.at[slot], csem.at[slot])

    def d_copy(p):
        slot = p % ND
        if p < 8:
            src = sd_ref.at[pl.ds((p % 2) * ff, ff), pl.ds((p // 2) * cw, cw)]
        else:
            q = p - 8
            src = ed_ref.at[q % 4, :, pl.ds((q // 4) * cw, cw)]
        return pltpu.make_async_copy(src, dbuf.at[slot], dsem.at[slot])

    g_copy(0).start()
    g_copy(1).start()
    g_copy(2).start()
    uk_copy().start()
    dkv_copy().start()
    c_copy(0, 0).start()
    c_copy(1, 1).start()
    g_copy(3).start()
    for i in range(4):
        uv_copy(i).start()
    g_copy(4).start()

    barrier = pltpu.get_barrier_semaphore()
    peers = [core_peer, y_peer, z_peers[1], z_peers[2], z_peers[3]]
    for peer in peers:
        pl.semaphore_signal(barrier, inc=1, device_id={"ep": peer}, device_id_type=MESH)

    lane = lax.broadcasted_iota(jnp.int32, (num_seq, 128), 1)
    member = jnp.zeros((num_seq, 128), F32)
    gate_te = jnp.zeros((num_seq, 128), F32)
    for k in range(top_k):
        hit = (lane % 64) == routes_ref[:, k:k + 1]
        member = jnp.where(hit, 1.0, member)
        gate_te = jnp.where(hit, rgate_ref[:, k:k + 1], gate_te)
    tri = jnp.where(lax.broadcasted_iota(jnp.int32, (num_seq, num_seq), 0) > lax.broadcasted_iota(jnp.int32, (num_seq, num_seq), 1), 1.0, 0.0)
    rank = jnp.dot(tri.astype(BF), member.astype(BF), preferred_element_type=F32)
    meta_own[...] = jnp.where(lane < 64, jnp.where(member > 0.5, rank, -4096.0), gate_te)

    freq = jnp.exp((lane % (rope // 2)).astype(F32) * (-2.0 * 9.210340371976184 / rope))
    angle = len_ref[...].astype(F32) * freq
    live = lane < rope
    cos_w = jnp.where(live, jnp.cos(angle), 0.0)
    sin_w = jnp.where(live, jnp.where(lane < rope // 2, -jnp.sin(angle), jnp.sin(angle)), 0.0)

    def rotate(v):
        turned = jnp.where(lane < rope // 2, pltpu.roll(v, 128 - rope // 2, 1), pltpu.roll(v, rope // 2, 1))
        return v * cos_w + turned * sin_w

    pl.semaphore_wait(barrier, len(peers))

    def ag(src_pos, peer, n, own, table):
        cc, yy, zz = src_pos
        idx = (cc * 2 + yy) * 4 + zz
        if table:
            mine_ref, all_ref, ss, rs = meta_own, meta_all, am_send, am_recv
        else:
            mine_ref, all_ref, ss, rs = h_own, h_all, ag_send, ag_recv
        return pltpu.make_async_remote_copy(src_ref=mine_ref if own else all_ref.at[cc, yy, zz], dst_ref=all_ref.at[cc, yy, zz], send_sem=ss.at[n], recv_sem=rs.at[idx], device_id={"ep": peer}, device_id_type=MESH)

    started = []

    def send(src_pos, peer, n, table, own=False):
        a = ag(src_pos, peer, n, own, table)
        a.start()
        started.append(a)

    def arrive(src_pos, table):
        ag(src_pos, core_peer, 0, False, table).wait_recv()

    mine = (c, y, z)

    def send_own(table):
        send(mine, y_peer, 0, table, True)
        for d in (1, 2, 3):
            send(mine, z_peers[d], d, table, True)
        send(mine, core_peer, 4, table, True)

    def fwd_z(d, table=False):
        pos = (c, y, zback[d])
        arrive(pos, table)
        send(pos, y_peer, 4 + d, table)
        send(pos, core_peer, 7 + d, table)

    def fwd_y(d, table=False):
        pos = (c, 1 - y, zback[d])
        arrive(pos, table)
        send(pos, core_peer, 11 + d, table)

    send_own(True)
    meta_all[c, y, z] = meta_own[...]

    def hidx(h):
        return h // 8, h // 4 % 2, h % 4

    def q_heads(k, first, count):
        g_copy(k).wait()
        qq = jnp.dot(x_ref[...], gbuf[k, :, pl.ds(0, count * qw)], preferred_element_type=F32).astype(BF).astype(F32)
        for i in range(count // 2):
            pair = qq[:, 2 * i * qw:2 * (i + 1) * qw]
            for h, v in ((first + 2 * i, pair), (first + 2 * i + 1, pltpu.roll(pair, qw, 1))):
                qn[h] = v[:, :nope].astype(BF)
                part[(*hidx(h), slice(None), pl.ds(latent, 128))] = rotate(v[:, nope:nope + 128])

    q_heads(0, 0, 6)
    g_copy(5).start()
    q_heads(1, 6, 6)
    g_copy(6).start()
    q_heads(2, 12, 4)
    uk_copy().wait()
    for h in range(num_heads):
        part[(*hidx(h), slice(None), pl.ds(0, latent))] = jnp.dot(qn[h], gbuf[2, pl.ds(h * nope, nope), pl.ds(W4, latent)], preferred_element_type=F32)
    g_copy(7).start()
    for d in (1, 2, 3):
        fwd_z(d, True)

    dkv_copy().wait()
    r = jnp.dot(x_ref[...], dkv_buf[...], preferred_element_type=F32)
    r_lat = r[:, :latent].astype(BF)
    r_rope = rotate(jnp.concatenate([r[:, latent:], jnp.zeros((num_seq, 128 - rope), F32)], axis=1)).astype(BF)
    kvf[:, :latent] = r_lat.astype(F32)
    kvf[:, latent:] = r_rope.astype(F32)
    kv_ref[:, :latent] = r_lat
    kv_ref[:, latent:] = r_rope[:, :rope]

    scale = qw ** -0.5
    nt = (((1,), (1,)), ((), ()))

    @pl.loop(0, num_seq // 8)
    def _(g):
        cs = lax.rem(g, 2)
        c_copy(g, cs).wait()
        rows8 = pl.ds(pl.multiple_of(g * 8, 8), 8)
        ql = part[:, :, :, rows8, pl.ds(0, latent)].reshape(128, latent).astype(BF)
        qr = part[:, :, :, rows8, pl.ds(latent, 128)].reshape(128, 128)[:, :rope].astype(BF)
        kv8 = kvf[rows8, :]
        lane8 = lax.broadcasted_iota(jnp.int32, (8, 128), 1)
        diag = lane8 % 8 == lax.broadcasted_iota(jnp.int32, (8, 128), 0)
        nrow = jnp.sum(jnp.where(diag, len_ref[rows8, :].astype(F32), 0.0), axis=0, keepdims=True)
        sn = lax.dot_general(kv8[:, :latent].astype(BF), ql, nt, preferred_element_type=F32) + lax.dot_general(kv8[:, latent:latent + rope].astype(BF), qr, nt, preferred_element_type=F32)
        s_new = jnp.sum(jnp.where(diag, sn, 0.0), axis=0, keepdims=True) * scale
        lane_l = lax.broadcasted_iota(jnp.int32, (256, 128), 1) % 8
        s = jnp.zeros((256, 128), F32)
        for half in range(2):
            kl = cbuf[cs, pl.ds(4 * half, 4), :, pl.ds(0, latent)].reshape(1024, latent)
            kr = cbuf[cs, pl.ds(4 * half, 4), :, pl.ds(latent, rope)].reshape(1024, rope)
            big = lax.dot_general(kl, ql, nt, preferred_element_type=F32) + lax.dot_general(kr, qr, nt, preferred_element_type=F32)
            for b in range(4):
                s = jnp.where(lane_l == 4 * half + b, big[b * 256:(b + 1) * 256], s)
        row_l = lax.broadcasted_iota(jnp.int32, (256, 128), 0).astype(F32)
        s = jnp.where(row_l < nrow, s * scale, -jnp.inf)
        top = jnp.maximum(jnp.max(s, axis=0, keepdims=True), s_new)
        e = jnp.exp(s - top)
        e_new = jnp.exp(s_new - top)
        den = jnp.sum(e, axis=0, keepdims=True) + e_new
        p = (e / den).T
        p_new = jnp.broadcast_to((e_new / den).astype(BF).astype(F32), (128, 128)).T
        row_p = lax.broadcasted_iota(jnp.int32, (128, 256), 0) % 8
        p_big = jnp.concatenate([jnp.where(row_p == b, p, 0.0).astype(BF) for b in range(8)], axis=1)
        o = jnp.dot(p_big, cbuf[cs, :, :, pl.ds(0, latent)].reshape(2048, latent), preferred_element_type=F32)
        kv_rep = jnp.broadcast_to(kv8[None, :, :latent], (16, 8, latent)).reshape(128, latent)
        o = o + jnp.concatenate([p_new] * (latent // 128), axis=1) * kv_rep
        part[:, :, :, rows8, pl.ds(1024, latent)] = o.reshape(2, 2, 4, 8, latent)

        @pl.when(g + 2 < num_seq // 8)
        def _():
            c_copy(g + 2, cs).start()

    for p in range(ND):
        d_copy(p).start()
    for d in range(4):
        fwd_y(d, True)
    for i in range(4):
        uv_copy(i).wait()
    g_copy(3).wait()
    for h in range(num_heads):
        ob = part[(*hidx(h), slice(None), pl.ds(1024, latent))].astype(BF)
        vcat[:, h * 128:(h + 1) * 128] = jnp.dot(ob, gbuf[3, pl.ds(h % 4 * latent, latent), pl.ds(OB + 128 * (h // 4), 128)], preferred_element_type=F32).astype(BF)
    g_copy(4).wait()
    for lo, hi, slot in ((0, ff, 4), (ff, hidden, 3)):
        a = jnp.dot(vcat[...], gbuf[slot, :, pl.ds(0, hi - lo)], preferred_element_type=F32).astype(BF)
        h_own[:, lo:hi] = (x_ref[:, lo:hi].astype(F32) + a.astype(F32)).astype(BF)
    g_copy(8).start()
    g_copy(9).start()
    send_own(False)
    h_all[c, y, z] = h_own[...]

    def gate_up(x, gslot, uslot, store):
        def block(start, size):
            g = jnp.dot(x(), gbuf[gslot, :, pl.ds(start, size)], preferred_element_type=F32)
            u = jnp.dot(x(), gbuf[uslot, :, pl.ds(start, size)], preferred_element_type=F32)
            store(start, size, (g * jax.nn.sigmoid(g) * u).astype(BF))

        @pl.loop(0, ff // 256)
        def _(n):
            block(pl.multiple_of(n * 256, 256), 256)

        if ff % 256:
            block(ff - ff % 256, ff % 256)

    def g_wait(k):
        g_copy(k).wait()

    for s in range(2):
        g_wait(2 * s + 5)
        g_wait(2 * s + 6)

        def put(start, size, v, s=s):
            act_sh[s, :, pl.ds(start, size)] = v
        gate_up(lambda: h_own[...], (2 * s + 5) % NG, (2 * s + 6) % NG, put)
        g_copy(2 * s + 10).start()
        g_copy(2 * s + 11).start()
        if s == 0:
            fwd_z(1)
            fwd_y(0)
        else:
            fwd_z(2)
            fwd_z(3)
    for j in range(NCH):
        d_copy(2 * j).wait()
        d_copy(2 * j + 1).wait()
        o = jnp.dot(act_sh[0], dbuf[2 * j], preferred_element_type=F32) + jnp.dot(act_sh[1], dbuf[2 * j + 1], preferred_element_type=F32)
        shared[:, j * cw:(j + 1) * cw] = o.astype(BF)
        d_copy(2 * j + 8).start()
        d_copy(2 * j + 9).start()
        if j >= 1:
            fwd_y(j)
    for yy in range(2):
        for zz in range(4):
            arrive((1 - c, yy, zz), True)
            arrive((1 - c, yy, zz), False)

    ntok = 16 * num_seq
    rows = 16 * 8
    meta = meta_all[...].reshape(ntok, 128)
    meta_t[...] = meta.T
    lane = lax.broadcasted_iota(jnp.int32, (ntok, 128), 1)
    base_col = lax.broadcasted_iota(jnp.int32, (ntok, 128), 0) // num_seq * 8
    base_row = lax.broadcasted_iota(jnp.int32, (1, ntok), 1) // num_seq * 8
    slot_row = lax.broadcasted_iota(jnp.int32, (rows, ntok), 0)
    for e in range(num_loc):
        ge = me * num_loc + e
        code = jnp.sum(jnp.where(lane == ge, meta, 0.0), axis=1, keepdims=True)
        gate = jnp.sum(jnp.where(lane == ge + 64, meta, 0.0), axis=1, keepdims=True)
        sel[e] = jnp.where(lane == code.astype(jnp.int32) + base_col, 1.0, 0.0).astype(BF)
        gates[e] = jnp.broadcast_to(gate, (ntok, 128))
        code_t = meta_t[pl.ds(ge, 1), :].astype(jnp.int32) + base_row
        sel_t[pl.ds(e * rows, rows), :] = jnp.where(slot_row == code_t, 1.0, 0.0).astype(BF)

    @pl.loop(0, hidden // 512)
    def _(n):
        cols = pl.ds(pl.multiple_of(n * 512, 512), 512)
        hh = h_all[:, :, :, :, cols].reshape(ntok, 512)
        xe[:, cols] = jnp.dot(sel_t[...], hh, preferred_element_type=F32).astype(BF)

    for e in range(num_loc):
        g_wait(9 + 2 * e)
        g_wait(10 + 2 * e)

        def put(start, size, v, e=e):
            act[e, :, pl.ds(start, size)] = v
        gate_up(lambda e=e: xe[pl.ds(e * rows, rows), :], (9 + 2 * e) % NG, (10 + 2 * e) % NG, put)
        for k in (14 + 2 * e, 15 + 2 * e):
            if k < 9 + 2 * num_loc:
                g_copy(k).start()

    def s1(j):
        cols = pl.ds(j * cw, cw)
        return pltpu.make_async_remote_copy(src_ref=part.at[1 - c, :, :, :, cols], dst_ref=rc.at[:, :, :, cols], send_sem=s1_send.at[j], recv_sem=s1_recv.at[j], device_id={"ep": core_peer}, device_id_type=MESH)

    def s2(j):
        cols = pl.ds(j * cw, cw)
        return pltpu.make_async_remote_copy(src_ref=part.at[c, 1 - y, :, :, cols], dst_ref=ry.at[:, :, cols], send_sem=s2_send.at[j], recv_sem=s2_recv.at[j], device_id={"ep": y_peer}, device_id_type=MESH)

    def s3(j, d):
        cols = pl.ds(j * cw, cw)
        return pltpu.make_async_remote_copy(src_ref=part.at[c, y, zs[d], :, cols], dst_ref=rz.at[d - 1, :, cols], send_sem=s3_send.at[j * 3 + d - 1], recv_sem=s3_recv.at[j * 3 + d - 1], device_id={"ep": z_peers[d]}, device_id_type=MESH)

    def after_s1(j):
        cols = slice(j * cw, (j + 1) * cw)
        s1(j).wait_recv()
        part[c, 1 - y, :, :, cols] = part[c, 1 - y, :, :, cols] + rc[1 - y, :, :, cols]
        s2(j).start()
        part[c, y, :, :, cols] = part[c, y, :, :, cols] + rc[y, :, :, cols]

    def after_s2(j):
        cols = slice(j * cw, (j + 1) * cw)
        s2(j).wait_recv()
        part[c, y, :, :, cols] = part[c, y, :, :, cols] + ry[:, :, cols]
        for d in (2, 1, 3):
            s3(j, d).start()

    def down(j):
        cols = pl.ds(j * cw, cw)
        for e in range(num_loc):
            p = 8 + 4 * j + e
            d_copy(p).wait()
        for e in range(num_loc):
            p = 8 + 4 * j + e
            o = jnp.dot(act[e], dbuf[p % ND], preferred_element_type=F32).astype(BF)
            if p + ND < 8 + 4 * NCH:
                d_copy(p + ND).start()
            for g in range(4):
                tok = pl.ds(g * ntok // 4, ntok // 4)
                b = jnp.dot(sel[e, tok, :], o, preferred_element_type=F32)
                gt = gates[e, tok, :]
                b = b * jnp.concatenate([gt] * (cw // 128), axis=1)
                b = b.reshape(4, num_seq, cw)
                if e == 0:
                    part[g // 2, g % 2, :, :, cols] = b
                else:
                    part[g // 2, g % 2, :, :, cols] = part[g // 2, g % 2, :, :, cols] + b

    for j in range(NCH):
        down(j)
        s1(j).start()
        if j >= 1:
            after_s1(j - 1)
        if j >= 2:
            after_s2(j - 2)
    after_s1(NCH - 1)
    after_s2(NCH - 2)
    after_s2(NCH - 1)
    for j in range(NCH):
        cols = slice(j * cw, (j + 1) * cw)
        for d in (1, 2, 3):
            s3(j, d).wait_recv()
        routed = part[c, y, z, :, cols] + rz[0, :, cols] + rz[1, :, cols] + rz[2, :, cols]
        out_ref[:, cols] = (h_own[:, cols].astype(F32) + shared[:, cols].astype(F32) + routed).astype(BF)
    for a in started:
        a.wait_send()
    for j in range(NCH):
        s1(j).wait_send()
        s2(j).wait_send()
        for d in (1, 2, 3):
            s3(j, d).wait_send()


def layer(x, lens, routes, route_gates, cache, w_q, w_dkv, w_uk, w_uv, w_o, sh_gate, sh_up, sh_down, ex_gate, ex_up, ex_down):
    num_seq, hidden = x.shape
    num_loc, _, ff = ex_gate.shape
    lat_row = cache.shape[2]
    ntok = 16 * num_seq
    dma = pltpu.SemaphoreType.DMA
    vm = pl.BlockSpec(memory_space=pltpu.VMEM)
    hbm = pl.BlockSpec(memory_space=pl.ANY)
    return pl.pallas_call(
        layer_kernel,
        out_shape=(jax.ShapeDtypeStruct((num_seq, hidden), BF), jax.ShapeDtypeStruct((num_seq, lat_row), BF)),
        in_specs=[vm] * 4 + [hbm] * 12,
        out_specs=(vm, vm),
        scratch_shapes=[
            pltpu.VMEM((NG, hidden, ff), BF),
            pltpu.VMEM((ND, ff, hidden // NCH), BF),
            pltpu.VMEM((2, 8, cache.shape[1], lat_row), BF),
            pltpu.VMEM((hidden, lat_row), BF),
            pltpu.VMEM((16, num_seq, 128), BF),
            pltpu.VMEM((num_seq, 640), F32),
            pltpu.VMEM((num_seq, hidden), BF),
            pltpu.VMEM((num_seq, hidden), BF),
            pltpu.VMEM((num_seq, 128), F32),
            pltpu.VMEM((2, 2, 4, num_seq, hidden), BF),
            pltpu.VMEM((2, 2, 4, num_seq, 128), F32),
            pltpu.VMEM((128, ntok), F32),
            pltpu.VMEM((num_loc, ntok, 128), BF),
            pltpu.VMEM((num_loc * 128, ntok), BF),
            pltpu.VMEM((num_loc, ntok, 128), F32),
            pltpu.VMEM((num_loc * 128, hidden), BF),
            pltpu.VMEM((num_loc, 128, ff), BF),
            pltpu.VMEM((2, num_seq, ff), BF),
            pltpu.VMEM((num_seq, hidden), BF),
            pltpu.VMEM((2, 2, 4, num_seq, hidden), F32),
            pltpu.VMEM((2, 4, num_seq, hidden), F32),
            pltpu.VMEM((4, num_seq, hidden), F32),
            pltpu.VMEM((3, num_seq, hidden), F32),
            dma((NG,)), dma((ND,)), dma((2,)), dma((6,)), dma((15,)), dma((16,)), dma((15,)), dma((16,)),
            dma((NCH,)), dma((NCH,)), dma((NCH,)), dma((NCH,)), dma((3 * NCH,)), dma((3 * NCH,)),
        ],
        compiler_params=pltpu.CompilerParams(collective_id=0, has_side_effects=True, vmem_limit_bytes=67043328),
        name="layer",
    )(x, lens, routes, route_gates, cache, w_q, w_dkv, w_uk, w_uv, w_o, sh_gate, sh_up, sh_down, ex_gate, ex_up, ex_down)


def solution(mesh):
    def device_step(x_blk, cache_blk, len_blk, routes, route_gates, w_q, w_dkv, w_uk, w_uv, w_o, sh_gate, sh_up, sh_down, ex_gate, ex_up, ex_down):
        lens = jnp.broadcast_to(len_blk[:, None], (len_blk.shape[0], 128))
        uk = w_uk.reshape(-1, w_uk.shape[2])
        uv = w_uv.reshape(-1, w_uv.shape[2])
        return layer(x_blk, lens, routes, route_gates, cache_blk, w_q, w_dkv, uk, uv, w_o, sh_gate, sh_up, sh_down, ex_gate, ex_up, ex_down)

    batch_spec = P(("dp", "ep"))
    weight_spec = P()
    expert_spec = P("ep")
    in_specs = (batch_spec,) * 5 + (weight_spec,) * 8 + (expert_spec,) * 3
    return jax.shard_map(device_step, mesh=mesh, in_specs=in_specs, out_specs=(batch_spec, batch_spec), check_vma=False)
```

```python
import functools

import jax
import jax.numpy as jnp
from jax import lax
from jax.experimental import pallas as pl
from jax.experimental.pallas import tpu as pltpu
from jax.sharding import PartitionSpec as P

MESH = pl.DeviceIdType.MESH
BF = jnp.bfloat16
F32 = jnp.float32


NG = 5
ND = 8
NCH = 4


def layer_kernel(x_ref, len_ref, routes_ref, rgate_ref, cache_ref, wq_ref, wdkv_ref, wuk_ref, wuv_ref, wo_ref,
                 sg_ref, su_ref, sd_ref, eg_ref, eu_ref, ed_ref, out_ref, kv_ref,
                 gbuf, dbuf, cbuf, dkv_buf, qn, kvf, lenb, vcat, h_own, meta_own,
                 h_all, meta_all, meta_t, sel, sel_t, gates, xe, act, act_sh, shared,
                 part, rc, ry, rz,
                 gsem, dsem, csem, xsem, ag_send, ag_recv, am_send, am_recv,
                 s1_send, s1_recv, s2_send, s2_recv, s3_send, s3_recv):
    me = lax.axis_index("ep")
    c = lax.rem(me, 2)
    y = lax.rem(lax.div(me, 2), 2)
    z = lax.div(me, 4)
    core_peer = me + 1 - 2 * c
    y_peer = me + 2 - 4 * y
    zs = [lax.rem(z + d, 4) for d in range(4)]
    zback = [lax.rem(z + 4 - d, 4) for d in range(4)]
    z_peers = [me + 4 * (zs[d] - z) for d in range(4)]
    num_loc, hidden, ff = eg_ref.shape
    num_seq = x_ref.shape[0]
    cw = hidden // NCH
    latent = wuk_ref.shape[1]
    num_heads = part.shape[0] * part.shape[1] * part.shape[2]
    nope = wuk_ref.shape[0] // num_heads
    rope = wdkv_ref.shape[0] - latent
    qw = nope + rope
    top_k = routes_ref.shape[0]

    W6 = 6 * qw
    W4 = 4 * qw
    OB = hidden - ff

    def g_copy(k):
        slot = k % NG
        dst = gbuf.at[slot]
        if k < 2:
            src, dst = wq_ref.at[:, pl.ds(k * W6, W6)], gbuf.at[slot, :, pl.ds(0, W6)]
        elif k == 2:
            src, dst = wq_ref.at[:, pl.ds(2 * W6, W4)], gbuf.at[slot, :, pl.ds(0, W4)]
        elif k == 3:
            src, dst = wo_ref.at[:, pl.ds(ff, OB)], gbuf.at[slot, :, pl.ds(0, OB)]
        elif k == 4:
            src = wo_ref.at[:, pl.ds(0, ff)]
        elif k < 9:
            src = (su_ref, sg_ref)[k % 2].at[:, pl.ds((k - 5) // 2 * ff, ff)]
        else:
            src = (eu_ref, eg_ref)[k % 2].at[(k - 9) // 2]
        return pltpu.make_async_copy(src, dst, gsem.at[slot])

    def uk_copy():
        return pltpu.make_async_copy(wuk_ref, gbuf.at[2, :, pl.ds(W4, latent)], xsem.at[0])

    def uv_copy(i):
        return pltpu.make_async_copy(wuv_ref.at[pl.ds(i * hidden, hidden)], gbuf.at[3, :, pl.ds(OB + 128 * i, 128)], xsem.at[1 + i])

    def dkv_copy():
        return pltpu.make_async_copy(wdkv_ref, dkv_buf, xsem.at[5])

    def c_copy(g, slot):
        return pltpu.make_async_copy(cache_ref.at[pl.ds(g * 8, 8)], cbuf.at[slot], csem.at[slot])

    def d_copy(p):
        slot = p % ND
        if p < 8:
            src = sd_ref.at[pl.ds((p % 2) * ff, ff), pl.ds((p // 2) * cw, cw)]
        else:
            q = p - 8
            src = ed_ref.at[q % 4, :, pl.ds((q // 4) * cw, cw)]
        return pltpu.make_async_copy(src, dbuf.at[slot], dsem.at[slot])

    g_copy(0).start()
    g_copy(1).start()
    g_copy(2).start()
    uk_copy().start()
    dkv_copy().start()
    c_copy(0, 0).start()
    c_copy(1, 1).start()
    g_copy(3).start()
    for i in range(4):
        uv_copy(i).start()
    g_copy(4).start()

    barrier = pltpu.get_barrier_semaphore()
    peers = [core_peer, y_peer, z_peers[1], z_peers[2], z_peers[3]]
    for peer in peers:
        pl.semaphore_signal(barrier, inc=1, device_id={"ep": peer}, device_id_type=MESH)

    lane = lax.broadcasted_iota(jnp.int32, (num_seq, 128), 1)
    pad_k = jnp.zeros((8 - top_k, num_seq), F32)
    small = jnp.concatenate([routes_ref[...].astype(F32), pad_k, rgate_ref[...], pad_k, len_ref[...].astype(F32), jnp.zeros((15, num_seq), F32)], axis=0)
    small = jnp.concatenate([small, jnp.zeros((32, 128 - num_seq), F32)], axis=1)
    cols = jnp.concatenate([small, jnp.zeros((96, 128), F32)], axis=0).T[:num_seq]
    lenb[...] = jnp.broadcast_to(cols[:, 16:17], (num_seq, 128))
    member = jnp.zeros((num_seq, 128), F32)
    gate_te = jnp.zeros((num_seq, 128), F32)
    for k in range(top_k):
        hit = (lane % 64).astype(F32) == cols[:, k:k + 1]
        member = jnp.where(hit, 1.0, member)
        gate_te = jnp.where(hit, cols[:, 8 + k:9 + k], gate_te)
    tri = jnp.where(lax.broadcasted_iota(jnp.int32, (num_seq, num_seq), 0) > lax.broadcasted_iota(jnp.int32, (num_seq, num_seq), 1), 1.0, 0.0)
    rank = jnp.dot(tri.astype(BF), member.astype(BF), preferred_element_type=F32)
    meta_own[...] = jnp.where(lane < 64, jnp.where(member > 0.5, rank, -4096.0), gate_te)

    freq = jnp.exp((lane % (rope // 2)).astype(F32) * (-2.0 * 9.210340371976184 / rope))
    angle = lenb[...] * freq
    live = lane < rope
    cos_w = jnp.where(live, jnp.cos(angle), 0.0)
    sin_w = jnp.where(live, jnp.where(lane < rope // 2, -jnp.sin(angle), jnp.sin(angle)), 0.0)

    def rotate(v):
        turned = jnp.where(lane < rope // 2, pltpu.roll(v, 128 - rope // 2, 1), pltpu.roll(v, rope // 2, 1))
        return v * cos_w + turned * sin_w

    pl.semaphore_wait(barrier, len(peers))

    def ag(src_pos, peer, n, own, table):
        cc, yy, zz = src_pos
        idx = (cc * 2 + yy) * 4 + zz
        if table:
            mine_ref, all_ref, ss, rs = meta_own, meta_all, am_send, am_recv
        else:
            mine_ref, all_ref, ss, rs = h_own, h_all, ag_send, ag_recv
        return pltpu.make_async_remote_copy(src_ref=mine_ref if own else all_ref.at[cc, yy, zz], dst_ref=all_ref.at[cc, yy, zz], send_sem=ss.at[n], recv_sem=rs.at[idx], device_id={"ep": peer}, device_id_type=MESH)

    started = []

    def send(src_pos, peer, n, table, own=False):
        a = ag(src_pos, peer, n, own, table)
        a.start()
        started.append(a)

    def arrive(src_pos, table):
        ag(src_pos, core_peer, 0, False, table).wait_recv()

    mine = (c, y, z)

    def send_own(table):
        send(mine, y_peer, 0, table, True)
        for d in (1, 2, 3):
            send(mine, z_peers[d], d, table, True)
        send(mine, core_peer, 4, table, True)

    def fwd_z(d, table=False):
        pos = (c, y, zback[d])
        arrive(pos, table)
        send(pos, y_peer, 4 + d, table)
        send(pos, core_peer, 7 + d, table)

    def fwd_y(d, table=False):
        pos = (c, 1 - y, zback[d])
        arrive(pos, table)
        send(pos, core_peer, 11 + d, table)

    send_own(True)
    meta_all[c, y, z] = meta_own[...]

    def hidx(h):
        return h // 8, h // 4 % 2, h % 4

    def q_heads(k, first, count):
        g_copy(k).wait()
        qq = jnp.dot(x_ref[...], gbuf[k, :, pl.ds(0, count * qw)], preferred_element_type=F32).astype(BF).astype(F32)
        for i in range(count // 2):
            pair = qq[:, 2 * i * qw:2 * (i + 1) * qw]
            for h, v in ((first + 2 * i, pair), (first + 2 * i + 1, pltpu.roll(pair, qw, 1))):
                qn[h] = v[:, :nope].astype(BF)
                part[(*hidx(h), slice(None), pl.ds(latent, 128))] = rotate(v[:, nope:nope + 128])

    q_heads(0, 0, 6)
    g_copy(5).start()
    q_heads(1, 6, 6)
    g_copy(6).start()
    q_heads(2, 12, 4)
    uk_copy().wait()
    for h in range(num_heads):
        part[(*hidx(h), slice(None), pl.ds(0, latent))] = jnp.dot(qn[h], gbuf[2, pl.ds(h * nope, nope), pl.ds(W4, latent)], preferred_element_type=F32)
    g_copy(7).start()
    for d in (1, 2, 3):
        fwd_z(d, True)

    nt = (((1,), (1,)), ((), ()))
    dkv_copy().wait()
    r = lax.dot_general(x_ref[...], dkv_buf[...], nt, preferred_element_type=F32)
    r_lat = r[:, :latent].astype(BF)
    r_rope = rotate(jnp.concatenate([r[:, latent:], jnp.zeros((num_seq, 128 - rope), F32)], axis=1)).astype(BF)
    kvf[:, :latent] = r_lat.astype(F32)
    kvf[:, latent:] = r_rope.astype(F32)
    kv_ref[:, :latent] = r_lat
    kv_ref[:, latent:] = r_rope[:, :rope]

    scale = qw ** -0.5

    @pl.loop(0, num_seq // 8)
    def _(g):
        cs = lax.rem(g, 2)
        c_copy(g, cs).wait()
        rows8 = pl.ds(pl.multiple_of(g * 8, 8), 8)
        q = part[:, :, :, rows8, pl.ds(0, latent + 128)].reshape(128, latent + 128).astype(BF)
        kv_rep = jnp.broadcast_to(kvf[rows8, :][None], (16, 8, latent + 128)).reshape(128, latent + 128)
        n_rep = jnp.broadcast_to(lenb[rows8, :][None], (16, 8, 128)).reshape(128, 128)
        n_rep = jnp.concatenate([n_rep, n_rep], axis=1)
        row = lax.broadcasted_iota(jnp.int32, (128, 256), 0) % 8
        pos = lax.broadcasted_iota(jnp.int32, (128, 256), 1).astype(F32)
        s_new = jnp.sum(q.astype(F32) * kv_rep, axis=1, keepdims=True) * scale
        q = q[:, :latent + rope]
        s = jnp.zeros((128, 256), F32)
        for b in range(8):
            s = jnp.where(row == b, jnp.dot(q, cbuf[cs, b], preferred_element_type=F32), s)
        s = jnp.where(pos < n_rep, s * scale, -jnp.inf)
        top = jnp.maximum(jnp.max(s, axis=1, keepdims=True), s_new)
        e = jnp.exp(s - top)
        e_new = jnp.exp(s_new - top)
        den = jnp.sum(e, axis=1, keepdims=True) + e_new
        p = e / den
        o = (e_new / den).astype(BF).astype(F32) * kv_rep[:, :latent]
        for b in range(8):
            o = o + lax.dot_general(jnp.where(row == b, p, 0.0).astype(BF), cbuf[cs, b, pl.ds(0, latent), :], nt, preferred_element_type=F32)
        part[:, :, :, rows8, pl.ds(1024, latent)] = o.reshape(2, 2, 4, 8, latent)

        @pl.when(g + 2 < num_seq // 8)
        def _():
            c_copy(g + 2, cs).start()

    for p in range(ND):
        d_copy(p).start()
    for d in range(4):
        fwd_y(d, True)
    for i in range(4):
        uv_copy(i).wait()
    g_copy(3).wait()
    for h in range(num_heads):
        ob = part[(*hidx(h), slice(None), pl.ds(1024, latent))].astype(BF)
        vcat[:, h * 128:(h + 1) * 128] = jnp.dot(ob, gbuf[3, pl.ds(h % 4 * latent, latent), pl.ds(OB + 128 * (h // 4), 128)], preferred_element_type=F32).astype(BF)
    g_copy(4).wait()
    for lo, hi, slot in ((0, ff, 4), (ff, hidden, 3)):
        a = jnp.dot(vcat[...], gbuf[slot, :, pl.ds(0, hi - lo)], preferred_element_type=F32).astype(BF)
        h_own[:, lo:hi] = (x_ref[:, lo:hi].astype(F32) + a.astype(F32)).astype(BF)
    g_copy(8).start()
    g_copy(9).start()
    send_own(False)
    h_all[c, y, z] = h_own[...]

    def gate_up(x, gslot, uslot, store):
        def block(start, size):
            g = jnp.dot(x(), gbuf[gslot, :, pl.ds(start, size)], preferred_element_type=F32)
            u = jnp.dot(x(), gbuf[uslot, :, pl.ds(start, size)], preferred_element_type=F32)
            store(start, size, (g * jax.nn.sigmoid(g) * u).astype(BF))

        for start in range(0, ff, 512):
            block(start, min(512, ff - start))

    def g_wait(k):
        g_copy(k).wait()

    for s in range(2):
        g_wait(2 * s + 5)
        g_wait(2 * s + 6)

        def put(start, size, v, s=s):
            act_sh[s, :, pl.ds(start, size)] = v
        gate_up(lambda: h_own[...], (2 * s + 5) % NG, (2 * s + 6) % NG, put)
        g_copy(2 * s + 10).start()
        g_copy(2 * s + 11).start()
        if s == 0:
            fwd_z(1)
            fwd_y(0)
        else:
            fwd_z(2)
            fwd_z(3)
    for j in range(NCH):
        d_copy(2 * j).wait()
        d_copy(2 * j + 1).wait()
        o = jnp.dot(act_sh[0], dbuf[2 * j], preferred_element_type=F32) + jnp.dot(act_sh[1], dbuf[2 * j + 1], preferred_element_type=F32)
        shared[:, j * cw:(j + 1) * cw] = o.astype(BF)
        d_copy(2 * j + 8).start()
        d_copy(2 * j + 9).start()
        if j >= 1:
            fwd_y(j)
    for yy in range(2):
        for zz in range(4):
            arrive((1 - c, yy, zz), True)
            arrive((1 - c, yy, zz), False)

    ntok = 16 * num_seq
    rows = 16 * 8
    meta = meta_all[...].reshape(ntok, 128)
    meta_t[...] = meta.T
    lane = lax.broadcasted_iota(jnp.int32, (ntok, 128), 1)
    base_col = lax.broadcasted_iota(jnp.int32, (ntok, 128), 0) // num_seq * 8
    base_row = lax.broadcasted_iota(jnp.int32, (1, ntok), 1) // num_seq * 8
    slot_row = lax.broadcasted_iota(jnp.int32, (rows, ntok), 0)
    for e in range(num_loc):
        ge = me * num_loc + e
        code = jnp.sum(jnp.where(lane == ge, meta, 0.0), axis=1, keepdims=True)
        gate = jnp.sum(jnp.where(lane == ge + 64, meta, 0.0), axis=1, keepdims=True)
        sel[e] = jnp.where(lane == code.astype(jnp.int32) + base_col, 1.0, 0.0).astype(BF)
        gates[e] = jnp.broadcast_to(gate, (ntok, 128))
        code_t = meta_t[pl.ds(ge, 1), :].astype(jnp.int32) + base_row
        sel_t[pl.ds(e * rows, rows), :] = jnp.where(slot_row == code_t, 1.0, 0.0).astype(BF)

    @pl.loop(0, hidden // 512)
    def _(n):
        cols = pl.ds(pl.multiple_of(n * 512, 512), 512)
        hh = h_all[:, :, :, :, cols].reshape(ntok, 512)
        xe[:, cols] = jnp.dot(sel_t[...], hh, preferred_element_type=F32).astype(BF)

    for e in range(num_loc):
        g_wait(9 + 2 * e)
        g_wait(10 + 2 * e)

        def put(start, size, v, e=e):
            act[e, :, pl.ds(start, size)] = v
        gate_up(lambda e=e: xe[pl.ds(e * rows, rows), :], (9 + 2 * e) % NG, (10 + 2 * e) % NG, put)
        for k in (14 + 2 * e, 15 + 2 * e):
            if k < 9 + 2 * num_loc:
                g_copy(k).start()

    def s1(j):
        cols = pl.ds(j * cw, cw)
        return pltpu.make_async_remote_copy(src_ref=part.at[1 - c, :, :, :, cols], dst_ref=rc.at[:, :, :, cols], send_sem=s1_send.at[j], recv_sem=s1_recv.at[j], device_id={"ep": core_peer}, device_id_type=MESH)

    def s2(j):
        cols = pl.ds(j * cw, cw)
        return pltpu.make_async_remote_copy(src_ref=part.at[c, 1 - y, :, :, cols], dst_ref=ry.at[:, :, cols], send_sem=s2_send.at[j], recv_sem=s2_recv.at[j], device_id={"ep": y_peer}, device_id_type=MESH)

    def s3(j, d):
        cols = pl.ds(j * cw, cw)
        return pltpu.make_async_remote_copy(src_ref=part.at[c, y, zs[d], :, cols], dst_ref=rz.at[d - 1, :, cols], send_sem=s3_send.at[j * 3 + d - 1], recv_sem=s3_recv.at[j * 3 + d - 1], device_id={"ep": z_peers[d]}, device_id_type=MESH)

    def after_s1(j):
        cols = slice(j * cw, (j + 1) * cw)
        s1(j).wait_recv()
        part[c, 1 - y, :, :, cols] = part[c, 1 - y, :, :, cols] + rc[1 - y, :, :, cols]
        s2(j).start()
        part[c, y, :, :, cols] = part[c, y, :, :, cols] + rc[y, :, :, cols]

    def after_s2(j):
        cols = slice(j * cw, (j + 1) * cw)
        s2(j).wait_recv()
        part[c, y, :, :, cols] = part[c, y, :, :, cols] + ry[:, :, cols]
        for d in (2, 1, 3):
            s3(j, d).start()

    def down(j):
        cols = pl.ds(j * cw, cw)
        for e in range(num_loc):
            p = 8 + 4 * j + e
            d_copy(p).wait()
        for e in range(num_loc):
            p = 8 + 4 * j + e
            o = jnp.dot(act[e], dbuf[p % ND], preferred_element_type=F32).astype(BF)
            if p + ND < 8 + 4 * NCH:
                d_copy(p + ND).start()
            for g in range(4):
                tok = pl.ds(g * ntok // 4, ntok // 4)
                b = jnp.dot(sel[e, tok, :], o, preferred_element_type=F32)
                gt = gates[e, tok, :]
                b = b * jnp.concatenate([gt] * (cw // 128), axis=1)
                b = b.reshape(4, num_seq, cw)
                if e == 0:
                    part[g // 2, g % 2, :, :, cols] = b
                else:
                    part[g // 2, g % 2, :, :, cols] = part[g // 2, g % 2, :, :, cols] + b

    for j in range(NCH):
        down(j)
        s1(j).start()
        if j >= 1:
            after_s1(j - 1)
        if j >= 2:
            after_s2(j - 2)
    after_s1(NCH - 1)
    after_s2(NCH - 2)
    after_s2(NCH - 1)
    for j in range(NCH):
        cols = slice(j * cw, (j + 1) * cw)
        for d in (1, 2, 3):
            s3(j, d).wait_recv()
        routed = part[c, y, z, :, cols] + rz[0, :, cols] + rz[1, :, cols] + rz[2, :, cols]
        out_ref[:, cols] = (h_own[:, cols].astype(F32) + shared[:, cols].astype(F32) + routed).astype(BF)
    for a in started:
        a.wait_send()
    for j in range(NCH):
        s1(j).wait_send()
        s2(j).wait_send()
        for d in (1, 2, 3):
            s3(j, d).wait_send()


def layer(x, lens, routes, route_gates, cache, w_q, w_dkv, w_uk, w_uv, w_o, sh_gate, sh_up, sh_down, ex_gate, ex_up, ex_down):
    num_seq, hidden = x.shape
    num_loc, _, ff = ex_gate.shape
    lat_row = cache.shape[1]
    ntok = 16 * num_seq
    dma = pltpu.SemaphoreType.DMA
    vm = pl.BlockSpec(memory_space=pltpu.VMEM)
    hbm = pl.BlockSpec(memory_space=pl.ANY)
    return pl.pallas_call(
        layer_kernel,
        out_shape=(jax.ShapeDtypeStruct((num_seq, hidden), BF), jax.ShapeDtypeStruct((num_seq, lat_row), BF)),
        in_specs=[vm] * 4 + [hbm] * 12,
        out_specs=(vm, vm),
        scratch_shapes=[
            pltpu.VMEM((NG, hidden, ff), BF),
            pltpu.VMEM((ND, ff, hidden // NCH), BF),
            pltpu.VMEM((2, 8, lat_row, cache.shape[2]), BF),
            pltpu.VMEM((lat_row, hidden), BF),
            pltpu.VMEM((16, num_seq, 128), BF),
            pltpu.VMEM((num_seq, 640), F32),
            pltpu.VMEM((num_seq, 128), F32),
            pltpu.VMEM((num_seq, hidden), BF),
            pltpu.VMEM((num_seq, hidden), BF),
            pltpu.VMEM((num_seq, 128), F32),
            pltpu.VMEM((2, 2, 4, num_seq, hidden), BF),
            pltpu.VMEM((2, 2, 4, num_seq, 128), F32),
            pltpu.VMEM((128, ntok), F32),
            pltpu.VMEM((num_loc, ntok, 128), BF),
            pltpu.VMEM((num_loc * 128, ntok), BF),
            pltpu.VMEM((num_loc, ntok, 128), F32),
            pltpu.VMEM((num_loc * 128, hidden), BF),
            pltpu.VMEM((num_loc, 128, ff), BF),
            pltpu.VMEM((2, num_seq, ff), BF),
            pltpu.VMEM((num_seq, hidden), BF),
            pltpu.VMEM((2, 2, 4, num_seq, hidden), F32),
            pltpu.VMEM((2, 4, num_seq, hidden), F32),
            pltpu.VMEM((4, num_seq, hidden), F32),
            pltpu.VMEM((3, num_seq, hidden), F32),
            dma((NG,)), dma((ND,)), dma((2,)), dma((6,)), dma((15,)), dma((16,)), dma((15,)), dma((16,)),
            dma((NCH,)), dma((NCH,)), dma((NCH,)), dma((NCH,)), dma((3 * NCH,)), dma((3 * NCH,)),
        ],
        compiler_params=pltpu.CompilerParams(collective_id=0, has_side_effects=True, vmem_limit_bytes=67043328),
        name="layer",
    )(x, lens, routes, route_gates, cache, w_q, w_dkv, w_uk, w_uv, w_o, sh_gate, sh_up, sh_down, ex_gate, ex_up, ex_down)


def solution(mesh):
    def device_step(x_blk, cache_blk, len_blk, routes, route_gates, w_q, w_dkv, w_uk, w_uv, w_o, sh_gate, sh_up, sh_down, ex_gate, ex_up, ex_down):
        lens = len_blk[None, :]
        uk = w_uk.reshape(-1, w_uk.shape[2])
        uv = w_uv.reshape(-1, w_uv.shape[2])
        return layer(x_blk, lens, routes.T, route_gates.T, cache_blk.transpose(0, 2, 1), w_q, w_dkv.T, uk, uv, w_o, sh_gate, sh_up, sh_down, ex_gate, ex_up, ex_down)

    batch_spec = P(("dp", "ep"))
    weight_spec = P()
    expert_spec = P("ep")
    in_specs = (batch_spec,) * 5 + (weight_spec,) * 8 + (expert_spec,) * 3
    return jax.shard_map(device_step, mesh=mesh, in_specs=in_specs, out_specs=(batch_spec, batch_spec), check_vma=False)
```

```python
import functools

import jax
import jax.numpy as jnp
from jax import lax
from jax.experimental import pallas as pl
from jax.experimental.pallas import tpu as pltpu
from jax.sharding import PartitionSpec as P

MESH = pl.DeviceIdType.MESH
BF = jnp.bfloat16
F32 = jnp.float32


NG = 5
ND = 8
NCH = 8
NA = 2


def layer_kernel(x_ref, len_ref, routes_ref, rgate_ref, cache_ref, wq_ref, wdkv_ref, wuk_ref, wuv_ref, wo_ref,
                 sg_ref, su_ref, sd_ref, eg_ref, eu_ref, ed_ref, out_ref, kv_ref,
                 gbuf, dbuf, cbuf, dkv_buf, qn, kvf, lenb, vcat, h_own, meta_own,
                 h_all, meta_all, meta_t, sel, sel_t, gates, xe, act, act_sh, shared,
                 part, rc, ry, rz,
                 gsem, dsem, csem, xsem, ag_send, ag_recv, am_send, am_recv,
                 s1_send, s1_recv, s2_send, s2_recv, s3_send, s3_recv, s4_send, s4_recv):
    me = lax.axis_index("ep")
    c = lax.rem(me, 2)
    y = lax.rem(lax.div(me, 2), 2)
    z = lax.div(me, 4)
    core_peer = me + 1 - 2 * c
    y_peer = me + 2 - 4 * y
    za = z + 1 - 2 * lax.rem(z, 2)
    zb = z + 2 - 4 * lax.div(z, 2)
    zc = za + zb - z
    za_peer = me + 4 * (za - z)
    zb_peer = me + 4 * (zb - z)
    num_loc, hidden, ff = eg_ref.shape
    num_seq = x_ref.shape[0]
    cw = hidden // NCH
    dw = 2 * cw
    aw = hidden // NA
    latent = wuk_ref.shape[1]
    num_heads = part.shape[0] * part.shape[1] * part.shape[2]
    nope = wuk_ref.shape[0] // num_heads
    rope = wdkv_ref.shape[0] - latent
    qw = nope + rope
    top_k = routes_ref.shape[0]

    W6 = 6 * qw
    W4 = 4 * qw
    OB = hidden - ff

    def g_copy(k):
        slot = k % NG
        dst = gbuf.at[slot]
        if k < 2:
            src, dst = wq_ref.at[:, pl.ds(k * W6, W6)], gbuf.at[slot, :, pl.ds(0, W6)]
        elif k == 2:
            src, dst = wq_ref.at[:, pl.ds(2 * W6, W4)], gbuf.at[slot, :, pl.ds(0, W4)]
        elif k == 3:
            src, dst = wo_ref.at[:, pl.ds(ff, OB)], gbuf.at[slot, :, pl.ds(0, OB)]
        elif k == 4:
            src = wo_ref.at[:, pl.ds(0, ff)]
        elif k < 13:
            src = (eu_ref, eg_ref)[k % 2].at[(k - 5) // 2]
        else:
            src = (su_ref, sg_ref)[k % 2].at[:, pl.ds((k - 13) // 2 * ff, ff)]
        return pltpu.make_async_copy(src, dst, gsem.at[slot])

    def uk_copy():
        return pltpu.make_async_copy(wuk_ref, gbuf.at[2, :, pl.ds(W4, latent)], xsem.at[0])

    def uv_copy(i):
        return pltpu.make_async_copy(wuv_ref.at[pl.ds(i * hidden, hidden)], gbuf.at[3, :, pl.ds(OB + 128 * i, 128)], xsem.at[1 + i])

    def dkv_copy():
        return pltpu.make_async_copy(wdkv_ref, dkv_buf, xsem.at[5])

    def c_copy(g, slot):
        return pltpu.make_async_copy(cache_ref.at[pl.ds(g * 8, 8)], cbuf.at[slot], csem.at[slot])

    def d_copy(p):
        slot = p % ND
        if p < 16:
            src = ed_ref.at[p % 4, :, pl.ds((p // 4) * dw, dw)]
        else:
            q = p - 16
            src = sd_ref.at[pl.ds((q % 2) * ff, ff), pl.ds((q // 2) * dw, dw)]
        return pltpu.make_async_copy(src, dbuf.at[slot], dsem.at[slot])

    g_copy(0).start()
    g_copy(1).start()
    g_copy(2).start()
    uk_copy().start()
    dkv_copy().start()
    c_copy(0, 0).start()
    c_copy(1, 1).start()
    g_copy(3).start()
    for i in range(4):
        uv_copy(i).start()
    g_copy(4).start()

    barrier = pltpu.get_barrier_semaphore()
    peers = [core_peer, y_peer, za_peer, zb_peer]
    for peer in peers:
        pl.semaphore_signal(barrier, inc=1, device_id={"ep": peer}, device_id_type=MESH)

    lane = lax.broadcasted_iota(jnp.int32, (num_seq, 128), 1)
    pad_k = jnp.zeros((8 - top_k, num_seq), F32)
    small = jnp.concatenate([routes_ref[...].astype(F32), pad_k, rgate_ref[...], pad_k, len_ref[...].astype(F32), jnp.zeros((15, num_seq), F32)], axis=0)
    small = jnp.concatenate([small, jnp.zeros((32, 128 - num_seq), F32)], axis=1)
    cols = jnp.concatenate([small, jnp.zeros((96, 128), F32)], axis=0).T[:num_seq]
    lenb[...] = jnp.broadcast_to(cols[:, 16:17], (num_seq, 128))
    member = jnp.zeros((num_seq, 128), F32)
    gate_te = jnp.zeros((num_seq, 128), F32)
    for k in range(top_k):
        hit = (lane % 64).astype(F32) == cols[:, k:k + 1]
        member = jnp.where(hit, 1.0, member)
        gate_te = jnp.where(hit, cols[:, 8 + k:9 + k], gate_te)
    tri = jnp.where(lax.broadcasted_iota(jnp.int32, (num_seq, num_seq), 0) > lax.broadcasted_iota(jnp.int32, (num_seq, num_seq), 1), 1.0, 0.0)
    rank = jnp.dot(tri.astype(BF), member.astype(BF), preferred_element_type=F32)
    meta_own[...] = jnp.where(lane < 64, jnp.where(member > 0.5, rank, -4096.0), gate_te)

    freq = jnp.exp((lane % (rope // 2)).astype(F32) * (-2.0 * 9.210340371976184 / rope))
    angle = lenb[...] * freq
    live = lane < rope
    cos_w = jnp.where(live, jnp.cos(angle), 0.0)
    sin_w = jnp.where(live, jnp.where(lane < rope // 2, -jnp.sin(angle), jnp.sin(angle)), 0.0)

    def rotate(v):
        turned = jnp.where(lane < rope // 2, pltpu.roll(v, 128 - rope // 2, 1), pltpu.roll(v, rope // 2, 1))
        return v * cos_w + turned * sin_w

    def ag(src_pos, peer, n, own, part_no):
        cc, yy, zz = src_pos
        idx = (cc * 2 + yy) * 4 + zz
        if part_no is None:
            src = meta_own if own else meta_all.at[cc, yy, zz]
            return pltpu.make_async_remote_copy(src_ref=src, dst_ref=meta_all.at[cc, yy, zz], send_sem=am_send.at[n], recv_sem=am_recv.at[idx], device_id={"ep": peer}, device_id_type=MESH)
        cols = pl.ds(part_no * aw, aw)
        src = h_own.at[:, cols] if own else h_all.at[cc, yy, zz, :, cols]
        return pltpu.make_async_remote_copy(src_ref=src, dst_ref=h_all.at[cc, yy, zz, :, cols], send_sem=ag_send.at[part_no * 15 + n], recv_sem=ag_recv.at[part_no * 16 + idx], device_id={"ep": peer}, device_id_type=MESH)

    started = []

    def send(src_pos, peer, n, part_no, own=False):
        a = ag(src_pos, peer, n, own, part_no)
        a.start()
        started.append(a)

    def arrive(src_pos, part_no):
        ag(src_pos, core_peer, 0, False, part_no).wait_recv()

    def send_own(part_no):
        for n, peer in enumerate((zb_peer, y_peer, za_peer, core_peer)):
            send((c, y, z), peer, n, part_no, True)

    def fwd_zb(part_no):
        pos = (c, y, zb)
        arrive(pos, part_no)
        send(pos, za_peer, 4, part_no)
        send(pos, y_peer, 5, part_no)
        send(pos, core_peer, 6, part_no)

    def fwd_za(part_no):
        pos = (c, y, za)
        arrive(pos, part_no)
        send(pos, y_peer, 7, part_no)
        send(pos, core_peer, 8, part_no)

    def fwd_zc(part_no):
        pos = (c, y, zc)
        arrive(pos, part_no)
        send(pos, y_peer, 9, part_no)
        send(pos, core_peer, 10, part_no)

    def fwd_y(i, part_no):
        pos = (c, 1 - y, (z, zb, za, zc)[i])
        arrive(pos, part_no)
        send(pos, core_peer, 11 + i, part_no)

    def hidx(h):
        return h // 8, h // 4 % 2, h % 4

    def q_heads(k, first, count):
        g_copy(k).wait()
        qq = jnp.dot(x_ref[...], gbuf[k, :, pl.ds(0, count * qw)], preferred_element_type=F32).astype(BF).astype(F32)
        for i in range(count // 2):
            pair = qq[:, 2 * i * qw:2 * (i + 1) * qw]
            for h, v in ((first + 2 * i, pair), (first + 2 * i + 1, pltpu.roll(pair, qw, 1))):
                qn[h] = v[:, :nope].astype(BF)
                part[(*hidx(h), slice(None), pl.ds(latent, 128))] = rotate(v[:, nope:nope + 128])

    q_heads(0, 0, 6)
    g_copy(5).start()
    q_heads(1, 6, 6)
    g_copy(6).start()
    q_heads(2, 12, 4)
    uk_copy().wait()
    for h in range(num_heads):
        part[(*hidx(h), slice(None), pl.ds(0, latent))] = jnp.dot(qn[h], gbuf[2, pl.ds(h * nope, nope), pl.ds(W4, latent)], preferred_element_type=F32)
    g_copy(7).start()

    nt = (((1,), (1,)), ((), ()))
    dkv_copy().wait()
    r = lax.dot_general(x_ref[...], dkv_buf[...], nt, preferred_element_type=F32)
    r_lat = r[:, :latent].astype(BF)
    r_rope = rotate(jnp.concatenate([r[:, latent:], jnp.zeros((num_seq, 128 - rope), F32)], axis=1)).astype(BF)
    kvf[:, :latent] = r_lat.astype(F32)
    kvf[:, latent:] = r_rope.astype(F32)
    kv_ref[:, :latent] = r_lat
    kv_ref[:, latent:] = r_rope[:, :rope]

    scale = qw ** -0.5

    @pl.loop(0, num_seq // 8)
    def _(g):
        cs = lax.rem(g, 2)
        c_copy(g, cs).wait()
        rows8 = pl.ds(pl.multiple_of(g * 8, 8), 8)
        q = part[:, :, :, rows8, pl.ds(0, latent + 128)].reshape(128, latent + 128).astype(BF)
        kv_rep = jnp.broadcast_to(kvf[rows8, :][None], (16, 8, latent + 128)).reshape(128, latent + 128)
        n_rep = jnp.broadcast_to(lenb[rows8, :][None], (16, 8, 128)).reshape(128, 128)
        n_rep = jnp.concatenate([n_rep, n_rep], axis=1)
        row = lax.broadcasted_iota(jnp.int32, (128, 256), 0) % 8
        pos = lax.broadcasted_iota(jnp.int32, (128, 256), 1).astype(F32)
        s_new = jnp.sum(q.astype(F32) * kv_rep, axis=1, keepdims=True) * scale
        q = q[:, :latent + rope]
        s = jnp.zeros((128, 256), F32)
        for b in range(8):
            s = jnp.where(row == b, jnp.dot(q, cbuf[cs, b], preferred_element_type=F32), s)
        s = jnp.where(pos < n_rep, s * scale, -jnp.inf)
        top = jnp.maximum(jnp.max(s, axis=1, keepdims=True), s_new)
        e = jnp.exp(s - top)
        e_new = jnp.exp(s_new - top)
        den = jnp.sum(e, axis=1, keepdims=True) + e_new
        p = e / den
        o = (e_new / den).astype(BF).astype(F32) * kv_rep[:, :latent]
        for b in range(8):
            o = o + lax.dot_general(jnp.where(row == b, p, 0.0).astype(BF), cbuf[cs, b, pl.ds(0, latent), :], nt, preferred_element_type=F32)
        part[:, :, :, rows8, pl.ds(1024, latent)] = o.reshape(2, 2, 4, 8, latent)

        @pl.when(g + 2 < num_seq // 8)
        def _():
            c_copy(g + 2, cs).start()

    for p in range(ND):
        d_copy(p).start()
    pl.semaphore_wait(barrier, len(peers))
    send_own(None)
    meta_all[c, y, z] = meta_own[...]
    for i in range(4):
        uv_copy(i).wait()
    g_copy(3).wait()
    for h in range(num_heads):
        ob = part[(*hidx(h), slice(None), pl.ds(1024, latent))].astype(BF)
        vcat[:, h * 128:(h + 1) * 128] = jnp.dot(ob, gbuf[3, pl.ds(h % 4 * latent, latent), pl.ds(OB + 128 * (h // 4), 128)], preferred_element_type=F32).astype(BF)
    fwd_zb(None)
    fwd_za(None)
    g_copy(4).wait()
    for lo, hi, slot in ((0, ff, 4), (ff, hidden, 3)):
        a = jnp.dot(vcat[...], gbuf[slot, :, pl.ds(0, hi - lo)], preferred_element_type=F32).astype(BF)
        h_own[:, lo:hi] = (x_ref[:, lo:hi].astype(F32) + a.astype(F32)).astype(BF)
        for i in range(NA):
            if lo < (i + 1) * aw <= hi:
                send_own(i)
    g_copy(8).start()
    g_copy(9).start()
    h_all[c, y, z] = h_own[...]
    fwd_zc(None)
    for i in range(4):
        fwd_y(i, None)
    fwd_za(0)
    fwd_zb(0)
    fwd_y(0, 0)
    fwd_za(1)
    fwd_zb(1)
    fwd_zc(0)
    fwd_y(0, 1)
    fwd_y(2, 0)
    fwd_y(1, 0)
    fwd_zc(1)

    def gate_up(x, gslot, uslot, store, starts=None):
        for start in starts or range(0, ff, 512):
            size = min(512, ff - start)
            g = jnp.dot(x(), gbuf[gslot, :, pl.ds(start, size)], preferred_element_type=F32)
            u = jnp.dot(x(), gbuf[uslot, :, pl.ds(start, size)], preferred_element_type=F32)
            store(start, size, (g * jax.nn.sigmoid(g) * u).astype(BF))

    def g_wait(k):
        g_copy(k).wait()

    for yy in range(2):
        for zz in range(4):
            arrive((1 - c, yy, zz), None)

    ntok = 16 * num_seq
    rows = 16 * 8
    meta = meta_all[...].reshape(ntok, 128)
    meta_t[...] = meta.T
    lane = lax.broadcasted_iota(jnp.int32, (ntok, 128), 1)
    base_col = lax.broadcasted_iota(jnp.int32, (ntok, 128), 0) // num_seq * 8
    base_row = lax.broadcasted_iota(jnp.int32, (1, ntok), 1) // num_seq * 8
    slot_row = lax.broadcasted_iota(jnp.int32, (rows, ntok), 0)
    for e in range(num_loc):
        ge = me * num_loc + e
        code = jnp.sum(jnp.where(lane == ge, meta, 0.0), axis=1, keepdims=True)
        gate = jnp.sum(jnp.where(lane == ge + 64, meta, 0.0), axis=1, keepdims=True)
        sel[e] = jnp.where(lane == code.astype(jnp.int32) + base_col, 1.0, 0.0).astype(BF)
        gates[e] = jnp.broadcast_to(gate, (ntok, 128))
        code_t = meta_t[pl.ds(ge, 1), :].astype(jnp.int32) + base_row
        sel_t[pl.ds(e * rows, rows), :] = jnp.where(slot_row == code_t, 1.0, 0.0).astype(BF)

    fwd_y(2, 1)
    fwd_y(1, 1)
    fwd_y(3, 0)
    fwd_y(3, 1)
    for i in range(NA):
        for yy in range(2):
            for zz in range(4):
                arrive((1 - c, yy, zz), i)

    @pl.loop(0, hidden // 512)
    def _(n):
        cols = pl.ds(pl.multiple_of(n * 512, 512), 512)
        hh = h_all[:, :, :, :, cols].reshape(ntok, 512)
        xe[:, cols] = jnp.dot(sel_t[...], hh, preferred_element_type=F32).astype(BF)

    for e in range(num_loc):
        g_wait(5 + 2 * e)
        g_wait(6 + 2 * e)

        def put(start, size, v, e=e):
            act[e, :, pl.ds(start, size)] = v
        gate_up(lambda e=e: xe[pl.ds(e * rows, rows), :], (5 + 2 * e) % NG, (6 + 2 * e) % NG, put)
        for k in (10 + 2 * e, 11 + 2 * e):
            if k < 17:
                g_copy(k).start()

    def rdma(src, dst, send_sem, recv_sem, peer):
        return pltpu.make_async_remote_copy(src_ref=src, dst_ref=dst, send_sem=send_sem, recv_sem=recv_sem, device_id={"ep": peer}, device_id_type=MESH)

    def chunk(j):
        return pl.ds(j * cw, cw)

    def s1(j):
        return rdma(part.at[1 - c, :, :, :, chunk(j)], rc.at[:, :, :, chunk(j)], s1_send.at[j], s1_recv.at[j], core_peer)

    def s2(j):
        return rdma(part.at[c, 1 - y, :, :, chunk(j)], ry.at[:, :, chunk(j)], s2_send.at[j], s2_recv.at[j], y_peer)

    def s3(j, i):
        return rdma(part.at[c, y, (zc, za)[i], :, chunk(j)], rz.at[i, :, chunk(j)], s3_send.at[2 * j + i], s3_recv.at[2 * j + i], za_peer)

    def s4(j):
        return rdma(part.at[c, y, zb, :, chunk(j)], rz.at[2, :, chunk(j)], s4_send.at[j], s4_recv.at[j], zb_peer)

    def step_a(j):
        cols = chunk(j)
        s1(j).wait_recv()
        part[c, 1 - y, :, :, cols] = part[c, 1 - y, :, :, cols] + rc[1 - y, :, :, cols]
        s2(j).start()
        part[c, y, :, :, cols] = part[c, y, :, :, cols] + rc[y, :, :, cols]

    def step_b(j):
        cols = chunk(j)
        s2(j).wait_recv()
        part[c, y, :, :, cols] = part[c, y, :, :, cols] + ry[:, :, cols]
        s3(j, 0).start()
        s3(j, 1).start()

    def step_c(j):
        cols = chunk(j)
        s3(j, 0).wait_recv()
        part[c, y, zb, :, cols] = part[c, y, zb, :, cols] + rz[0, :, cols]
        s4(j).start()

    def step_f(j):
        cols = chunk(j)
        s3(j, 1).wait_recv()
        s4(j).wait_recv()
        routed = part[c, y, z, :, cols] + rz[1, :, cols] + rz[2, :, cols]
        out_ref[:, cols] = (h_own[:, cols].astype(F32) + shared[:, cols].astype(F32) + routed).astype(BF)

    def down(j):
        cols = chunk(j)
        if j % 2 == 0:
            for e in range(num_loc):
                d_copy(2 * j + e).wait()
        for e in range(num_loc):
            slot = (j // 2 * 4 + e) % ND
            o = jnp.dot(act[e], dbuf[slot, :, pl.ds(j % 2 * cw, cw)], preferred_element_type=F32).astype(BF)
            b = jnp.dot(sel[e], o, preferred_element_type=F32)
            gt = gates[e]
            b = (b * jnp.concatenate([gt] * (cw // 128), axis=1)).reshape(2, 2, 4, num_seq, cw)
            if e == 0:
                part[:, :, :, :, cols] = b
            else:
                part[:, :, :, :, cols] = part[:, :, :, :, cols] + b
        if j % 2 == 1:
            for e in range(num_loc):
                d_copy(2 * (j - 1) + 8 + e).start()

    def shared_up(i):
        s, b = i // 3, i % 3
        if b == 0:
            g_wait(13 + 2 * s)
            g_wait(14 + 2 * s)

        def put(start, size, v):
            act_sh[s, :, pl.ds(start, size)] = v
        gate_up(lambda: h_own[...], (13 + 2 * s) % NG, (14 + 2 * s) % NG, put, (512 * b,))

    def shared_down(i):
        d_copy(16 + 2 * i).wait()
        d_copy(17 + 2 * i).wait()
        o = jnp.dot(act_sh[0], dbuf[2 * i], preferred_element_type=F32) + jnp.dot(act_sh[1], dbuf[2 * i + 1], preferred_element_type=F32)
        shared[:, i * dw:(i + 1) * dw] = o.astype(BF)

    for j in range(NCH):
        down(j)
        s1(j).start()
        if j >= 1:
            step_a(j - 1)
        if j == 6:
            step_b(0)
    step_a(NCH - 1)
    fill = [lambda i=i: shared_up(i) for i in range(6)] + [lambda i=i: shared_down(i) for i in range(4)]
    plan = [1, 2, 2, 2, 1, 1, 1]
    for j in range(1, NCH):
        step_b(j)
        for _ in range(plan[j - 1]):
            fill.pop(0)()
        step_c(j - 1)
        if j == NCH - 1:
            for i in range(NCH - 1):
                step_f(i)
    step_c(NCH - 1)
    step_f(NCH - 1)
    for a in started:
        a.wait_send()
    for j in range(NCH):
        s1(j).wait_send()
        s2(j).wait_send()
        s3(j, 0).wait_send()
        s3(j, 1).wait_send()
        s4(j).wait_send()


def layer(x, lens, routes, route_gates, cache, w_q, w_dkv, w_uk, w_uv, w_o, sh_gate, sh_up, sh_down, ex_gate, ex_up, ex_down):
    num_seq, hidden = x.shape
    num_loc, _, ff = ex_gate.shape
    lat_row = cache.shape[1]
    ntok = 16 * num_seq
    dma = pltpu.SemaphoreType.DMA
    vm = pl.BlockSpec(memory_space=pltpu.VMEM)
    hbm = pl.BlockSpec(memory_space=pl.ANY)
    return pl.pallas_call(
        layer_kernel,
        out_shape=(jax.ShapeDtypeStruct((num_seq, hidden), BF), jax.ShapeDtypeStruct((num_seq, lat_row), BF)),
        in_specs=[vm] * 4 + [hbm] * 12,
        out_specs=(vm, vm),
        scratch_shapes=[
            pltpu.VMEM((NG, hidden, ff), BF),
            pltpu.VMEM((ND, ff, 2 * hidden // NCH), BF),
            pltpu.VMEM((2, 8, lat_row, cache.shape[2]), BF),
            pltpu.VMEM((lat_row, hidden), BF),
            pltpu.VMEM((16, num_seq, 128), BF),
            pltpu.VMEM((num_seq, 640), F32),
            pltpu.VMEM((num_seq, 128), F32),
            pltpu.VMEM((num_seq, hidden), BF),
            pltpu.VMEM((num_seq, hidden), BF),
            pltpu.VMEM((num_seq, 128), F32),
            pltpu.VMEM((2, 2, 4, num_seq, hidden), BF),
            pltpu.VMEM((2, 2, 4, num_seq, 128), F32),
            pltpu.VMEM((128, ntok), F32),
            pltpu.VMEM((num_loc, ntok, 128), BF),
            pltpu.VMEM((num_loc * 128, ntok), BF),
            pltpu.VMEM((num_loc, ntok, 128), F32),
            pltpu.VMEM((num_loc * 128, hidden), BF),
            pltpu.VMEM((num_loc, 128, ff), BF),
            pltpu.VMEM((2, num_seq, ff), BF),
            pltpu.VMEM((num_seq, hidden), BF),
            pltpu.VMEM((2, 2, 4, num_seq, hidden), F32),
            pltpu.VMEM((2, 4, num_seq, hidden), F32),
            pltpu.VMEM((4, num_seq, hidden), F32),
            pltpu.VMEM((3, num_seq, hidden), F32),
            dma((NG,)), dma((ND,)), dma((2,)), dma((6,)), dma((15 * NA,)), dma((16 * NA,)), dma((15,)), dma((16,)),
            dma((NCH,)), dma((NCH,)), dma((NCH,)), dma((NCH,)), dma((2 * NCH,)), dma((2 * NCH,)), dma((NCH,)), dma((NCH,)),
        ],
        compiler_params=pltpu.CompilerParams(collective_id=0, has_side_effects=True, vmem_limit_bytes=67043328),
        name="layer",
    )(x, lens, routes, route_gates, cache, w_q, w_dkv, w_uk, w_uv, w_o, sh_gate, sh_up, sh_down, ex_gate, ex_up, ex_down)


def solution(mesh):
    def device_step(x_blk, cache_blk, len_blk, routes, route_gates, w_q, w_dkv, w_uk, w_uv, w_o, sh_gate, sh_up, sh_down, ex_gate, ex_up, ex_down):
        lens = len_blk[None, :]
        uk = w_uk.reshape(-1, w_uk.shape[2])
        uv = w_uv.reshape(-1, w_uv.shape[2])
        return layer(x_blk, lens, routes.T, route_gates.T, cache_blk.transpose(0, 2, 1), w_q, w_dkv.T, uk, uv, w_o, sh_gate, sh_up, sh_down, ex_gate, ex_up, ex_down)

    batch_spec = P(("dp", "ep"))
    weight_spec = P()
    expert_spec = P("ep")
    in_specs = (batch_spec,) * 5 + (weight_spec,) * 8 + (expert_spec,) * 3
    return jax.shard_map(device_step, mesh=mesh, in_specs=in_specs, out_specs=(batch_spec, batch_spec), check_vma=False)
```

```python
import functools

import jax
import jax.numpy as jnp
from jax import lax
from jax.experimental import pallas as pl
from jax.experimental.pallas import tpu as pltpu
from jax.sharding import PartitionSpec as P

MESH = pl.DeviceIdType.MESH
BF = jnp.bfloat16
F32 = jnp.float32


NG = 6
ND = 8
NCH = 8
NA = 2


def layer_kernel(x_ref, len_ref, routes_ref, rgate_ref, cache_ref, wq_ref, wdkv_ref, wuk_ref, wuv_ref, wo_ref,
                 sg_ref, su_ref, sd_ref, eg_ref, eu_ref, ed_ref, out_ref, kv_ref,
                 gbuf, dbuf, qn, kvf, lenb, vcat, h_own, meta_own,
                 h_all, meta_all, meta_t, sel, sel_t, gates, xe, act, act_sh, shared,
                 part, rc, ry, rz,
                 gsem, dsem, csem, xsem, ag_send, ag_recv, am_send, am_recv,
                 s1_send, s1_recv, s2_send, s2_recv, s3_send, s3_recv, s4_send, s4_recv):
    me = lax.axis_index("ep")
    c = lax.rem(me, 2)
    y = lax.rem(lax.div(me, 2), 2)
    z = lax.div(me, 4)
    core_peer = me + 1 - 2 * c
    y_peer = me + 2 - 4 * y
    za = z + 1 - 2 * lax.rem(z, 2)
    zb = z + 2 - 4 * lax.div(z, 2)
    zc = za + zb - z
    za_peer = me + 4 * (za - z)
    zb_peer = me + 4 * (zb - z)
    num_loc, hidden, ff = eg_ref.shape
    num_seq = x_ref.shape[0]
    cw = hidden // NCH
    dw = 2 * cw
    aw = hidden // NA
    latent = wuk_ref.shape[1]
    num_heads = part.shape[0] * part.shape[1] * part.shape[2]
    nope = wuk_ref.shape[0] // num_heads
    rope = wdkv_ref.shape[0] - latent
    qw = nope + rope
    top_k = routes_ref.shape[0]
    lat_row, cache_len = cache_ref.shape[1:]

    W6 = 6 * qw
    W4 = 4 * qw
    OB = hidden - ff

    def a_copy(k):
        if k < 2:
            src, dst = wq_ref.at[:, pl.ds(k * W6, W6)], gbuf.at[k, :, pl.ds(0, W6)]
        elif k == 2:
            src, dst = wq_ref.at[:, pl.ds(2 * W6, W4)], gbuf.at[k, :, pl.ds(0, W4)]
        elif k == 3:
            src, dst = wo_ref.at[:, pl.ds(ff, OB)], gbuf.at[k, :, pl.ds(0, OB)]
        else:
            src, dst = wo_ref.at[:, pl.ds(0, ff)], gbuf.at[k]
        return pltpu.make_async_copy(src, dst, gsem.at[k])

    def g_slot(m):
        return m % NG if m < 8 else m - 8

    def g_copy(m):
        if m < 8:
            src = (eg_ref, eu_ref)[m % 2].at[m // 2]
        else:
            src = (sg_ref, su_ref)[m % 2].at[:, pl.ds((m - 8) // 2 * ff, ff)]
        return pltpu.make_async_copy(src, gbuf.at[g_slot(m)], gsem.at[g_slot(m)])

    def uk_copy():
        return pltpu.make_async_copy(wuk_ref, gbuf.at[2, :, pl.ds(W4, latent)], xsem.at[0])

    def uv_copy(i):
        return pltpu.make_async_copy(wuv_ref.at[pl.ds(i * hidden, hidden)], gbuf.at[3, :, pl.ds(OB + 128 * i, 128)], xsem.at[1 + i])

    def dkv_copy(i):
        lo, size = ((0, ff), (ff, OB))[i]
        return pltpu.make_async_copy(wdkv_ref.at[:, pl.ds(lo, size)], gbuf.at[5, pl.ds(i * lat_row, lat_row), pl.ds(0, size)], xsem.at[5 + i])

    def cache_at(i, slot):
        return slot, pl.ds(i % 4 // 2 * lat_row, lat_row), pl.ds(i % 2 * cache_len, cache_len)

    def c_copy(i, seq, slot):
        return pltpu.make_async_copy(cache_ref.at[seq], dbuf.at[cache_at(i, slot)], csem.at[seq])

    def d_place(p):
        if 8 <= p < 16:
            return gbuf, (2 + (p - 8) // 2, pl.ds(0, ff), pl.ds(p % 2 * dw, dw))
        return dbuf, (p % ND, slice(None), slice(None))

    def d_copy(p):
        if p < 16:
            src = ed_ref.at[p % 4, :, pl.ds((p // 4) * dw, dw)]
        else:
            q = p - 16
            src = sd_ref.at[pl.ds((q % 2) * ff, ff), pl.ds((q // 2) * dw, dw)]
        buf, at = d_place(p)
        return pltpu.make_async_copy(src, buf.at[at], dsem.at[p % 16])

    for k in range(3):
        a_copy(k).start()
    uk_copy().start()
    dkv_copy(0).start()
    dkv_copy(1).start()
    for i in range(num_seq):
        c_copy(i, i, i // 4).start()
    a_copy(3).start()
    for i in range(4):
        uv_copy(i).start()
    a_copy(4).start()

    barrier = pltpu.get_barrier_semaphore()
    peers = [core_peer, y_peer, za_peer, zb_peer]
    for peer in peers:
        pl.semaphore_signal(barrier, inc=1, device_id={"ep": peer}, device_id_type=MESH)

    lane = lax.broadcasted_iota(jnp.int32, (num_seq, 128), 1)
    pad_k = jnp.zeros((8 - top_k, num_seq), F32)
    small = jnp.concatenate([routes_ref[...].astype(F32), pad_k, rgate_ref[...], pad_k, len_ref[...].astype(F32), jnp.zeros((15, num_seq), F32)], axis=0)
    small = jnp.concatenate([small, jnp.zeros((32, 128 - num_seq), F32)], axis=1)
    cols = jnp.concatenate([small, jnp.zeros((96, 128), F32)], axis=0).T[:num_seq]
    lenb[...] = jnp.broadcast_to(cols[:, 16:17], (num_seq, 128))
    member = jnp.zeros((num_seq, 128), F32)
    gate_te = jnp.zeros((num_seq, 128), F32)
    for k in range(top_k):
        hit = (lane % 64).astype(F32) == cols[:, k:k + 1]
        member = jnp.where(hit, 1.0, member)
        gate_te = jnp.where(hit, cols[:, 8 + k:9 + k], gate_te)
    tri = jnp.where(lax.broadcasted_iota(jnp.int32, (num_seq, num_seq), 0) > lax.broadcasted_iota(jnp.int32, (num_seq, num_seq), 1), 1.0, 0.0)
    rank = jnp.dot(tri.astype(BF), member.astype(BF), preferred_element_type=F32)
    meta_own[...] = jnp.where(lane < 64, jnp.where(member > 0.5, rank, -4096.0), gate_te)

    freq = jnp.exp((lane % (rope // 2)).astype(F32) * (-2.0 * 9.210340371976184 / rope))
    angle = lenb[...] * freq
    live = lane < rope
    cos_w = jnp.where(live, jnp.cos(angle), 0.0)
    sin_w = jnp.where(live, jnp.where(lane < rope // 2, -jnp.sin(angle), jnp.sin(angle)), 0.0)

    def rotate(v):
        turned = jnp.where(lane < rope // 2, pltpu.roll(v, 128 - rope // 2, 1), pltpu.roll(v, rope // 2, 1))
        return v * cos_w + turned * sin_w

    def ag(src_pos, peer, n, own, part_no):
        cc, yy, zz = src_pos
        idx = (cc * 2 + yy) * 4 + zz
        if part_no is None:
            src = meta_own if own else meta_all.at[cc, yy, zz]
            return pltpu.make_async_remote_copy(src_ref=src, dst_ref=meta_all.at[cc, yy, zz], send_sem=am_send.at[n], recv_sem=am_recv.at[idx], device_id={"ep": peer}, device_id_type=MESH)
        cols = pl.ds(part_no * aw, aw)
        src = h_own.at[:, cols] if own else h_all.at[cc, yy, zz, :, cols]
        return pltpu.make_async_remote_copy(src_ref=src, dst_ref=h_all.at[cc, yy, zz, :, cols], send_sem=ag_send.at[part_no * 15 + n], recv_sem=ag_recv.at[part_no * 16 + idx], device_id={"ep": peer}, device_id_type=MESH)

    started = []

    def send(src_pos, peer, n, part_no, own=False):
        a = ag(src_pos, peer, n, own, part_no)
        a.start()
        started.append(a)

    def arrive(src_pos, part_no):
        ag(src_pos, core_peer, 0, False, part_no).wait_recv()

    def send_own(part_no):
        for n, peer in enumerate((zb_peer, y_peer, za_peer, core_peer)):
            send((c, y, z), peer, n, part_no, True)

    def fwd_zb(part_no):
        pos = (c, y, zb)
        arrive(pos, part_no)
        send(pos, za_peer, 4, part_no)
        send(pos, y_peer, 5, part_no)
        send(pos, core_peer, 6, part_no)

    def fwd_za(part_no):
        pos = (c, y, za)
        arrive(pos, part_no)
        send(pos, y_peer, 7, part_no)
        send(pos, core_peer, 8, part_no)

    def fwd_zc(part_no):
        pos = (c, y, zc)
        arrive(pos, part_no)
        send(pos, y_peer, 9, part_no)
        send(pos, core_peer, 10, part_no)

    def fwd_y(i, part_no):
        pos = (c, 1 - y, (z, zb, za, zc)[i])
        arrive(pos, part_no)
        send(pos, core_peer, 11 + i, part_no)

    def hidx(h):
        return h // 8, h // 4 % 2, h % 4

    def q_heads(k, first, count):
        a_copy(k).wait()
        qq = jnp.dot(x_ref[...], gbuf[k, :, pl.ds(0, count * qw)], preferred_element_type=F32).astype(BF).astype(F32)
        for i in range(count // 2):
            pair = qq[:, 2 * i * qw:2 * (i + 1) * qw]
            for h, v in ((first + 2 * i, pair), (first + 2 * i + 1, pltpu.roll(pair, qw, 1))):
                qn[h] = v[:, :nope].astype(BF)
                part[(*hidx(h), slice(None), pl.ds(latent, 128))] = rotate(v[:, nope:nope + 128])

    q_heads(0, 0, 6)
    g_copy(0).start()
    q_heads(1, 6, 6)
    g_copy(1).start()
    q_heads(2, 12, 4)
    uk_copy().wait()
    for h in range(num_heads):
        part[(*hidx(h), slice(None), pl.ds(0, latent))] = jnp.dot(qn[h], gbuf[2, pl.ds(h * nope, nope), pl.ds(W4, latent)], preferred_element_type=F32)
    g_copy(2).start()
    pl.semaphore_wait(barrier, len(peers))
    send_own(None)
    meta_all[c, y, z] = meta_own[...]

    nt = (((1,), (1,)), ((), ()))
    dkv_copy(0).wait()
    dkv_copy(1).wait()
    r = lax.dot_general(x_ref[:, :ff], gbuf[5, pl.ds(0, lat_row), :], nt, preferred_element_type=F32) + lax.dot_general(x_ref[:, ff:], gbuf[5, pl.ds(lat_row, lat_row), pl.ds(0, OB)], nt, preferred_element_type=F32)
    g_copy(5).start()
    r_lat = r[:, :latent].astype(BF)
    r_rope = rotate(jnp.concatenate([r[:, latent:], jnp.zeros((num_seq, 128 - rope), F32)], axis=1)).astype(BF)
    kvf[:, :latent] = r_lat.astype(F32)
    kvf[:, latent:] = r_rope.astype(F32)
    kv_ref[:, :latent] = r_lat
    kv_ref[:, latent:] = r_rope[:, :rope]

    scale = qw ** -0.5

    @pl.loop(0, num_seq // 8)
    def _(g):
        for b in range(8):
            c_copy(b, g * 8 + b, 2 * g + b // 4).wait()
        rows8 = pl.ds(pl.multiple_of(g * 8, 8), 8)
        q = part[:, :, :, rows8, pl.ds(0, latent + 128)].reshape(128, latent + 128).astype(BF)
        kv_rep = jnp.broadcast_to(kvf[rows8, :][None], (16, 8, latent + 128)).reshape(128, latent + 128)
        n_rep = jnp.broadcast_to(lenb[rows8, :][None], (16, 8, 128)).reshape(128, 128)
        n_rep = jnp.concatenate([n_rep, n_rep], axis=1)
        row = lax.broadcasted_iota(jnp.int32, (128, 256), 0) % 8
        pos = lax.broadcasted_iota(jnp.int32, (128, 256), 1).astype(F32)
        s_new = jnp.sum(q.astype(F32) * kv_rep, axis=1, keepdims=True) * scale
        q = q[:, :latent + rope]
        s = jnp.zeros((128, 256), F32)
        for b in range(8):
            s = jnp.where(row == b, jnp.dot(q, dbuf[cache_at(b, 2 * g + b // 4)], preferred_element_type=F32), s)
        s = jnp.where(pos < n_rep, s * scale, -jnp.inf)
        top = jnp.maximum(jnp.max(s, axis=1, keepdims=True), s_new)
        e = jnp.exp(s - top)
        e_new = jnp.exp(s_new - top)
        den = jnp.sum(e, axis=1, keepdims=True) + e_new
        p = e / den
        o = (e_new / den).astype(BF).astype(F32) * kv_rep[:, :latent]
        for b in range(8):
            o = o + lax.dot_general(jnp.where(row == b, p, 0.0).astype(BF), dbuf[cache_at(b, 2 * g + b // 4)][:latent], nt, preferred_element_type=F32)
        part[:, :, :, rows8, pl.ds(1024, latent)] = o.reshape(2, 2, 4, 8, latent)

    for p in range(ND):
        d_copy(p).start()
    fwd_zb(None)
    fwd_za(None)
    for i in range(4):
        uv_copy(i).wait()
    a_copy(3).wait()
    for h in range(num_heads):
        ob = part[(*hidx(h), slice(None), pl.ds(1024, latent))].astype(BF)
        vcat[:, h * 128:(h + 1) * 128] = jnp.dot(ob, gbuf[3, pl.ds(h % 4 * latent, latent), pl.ds(OB + 128 * (h // 4), 128)], preferred_element_type=F32).astype(BF)
    a_copy(4).wait()
    fwd_zc(None)
    for lo, hi, slot in ((0, ff, 4), (ff, hidden, 3)):
        a = jnp.dot(vcat[...], gbuf[slot, :, pl.ds(0, hi - lo)], preferred_element_type=F32).astype(BF)
        h_own[:, lo:hi] = (x_ref[:, lo:hi].astype(F32) + a.astype(F32)).astype(BF)
        for i in range(NA):
            if lo < (i + 1) * aw <= hi:
                send_own(i)
    g_copy(3).start()
    g_copy(4).start()
    h_all[c, y, z] = h_own[...]
    for i in range(4):
        fwd_y(i, None)
    fwd_za(0)
    fwd_zb(0)
    fwd_y(0, 0)
    fwd_za(1)
    fwd_zb(1)
    fwd_zc(0)
    fwd_y(0, 1)
    fwd_y(2, 0)
    fwd_y(1, 0)
    fwd_zc(1)

    def gate_up(x, gslot, uslot, store, starts=None):
        for start in starts or range(0, ff, 512):
            size = min(512, ff - start)
            g = jnp.dot(x(), gbuf[gslot, :, pl.ds(start, size)], preferred_element_type=F32)
            u = jnp.dot(x(), gbuf[uslot, :, pl.ds(start, size)], preferred_element_type=F32)
            store(start, size, (g * jax.nn.sigmoid(g) * u).astype(BF))

    def g_wait(k):
        g_copy(k).wait()

    for yy in range(2):
        for zz in range(4):
            arrive((1 - c, yy, zz), None)

    ntok = 16 * num_seq
    rows = 16 * 8
    meta = meta_all[...].reshape(ntok, 128)
    meta_t[...] = meta.T
    lane = lax.broadcasted_iota(jnp.int32, (ntok, 128), 1)
    base_col = lax.broadcasted_iota(jnp.int32, (ntok, 128), 0) // num_seq * 8
    base_row = lax.broadcasted_iota(jnp.int32, (1, ntok), 1) // num_seq * 8
    slot_row = lax.broadcasted_iota(jnp.int32, (rows, ntok), 0)
    for e in range(num_loc):
        ge = me * num_loc + e
        code = jnp.sum(jnp.where(lane == ge, meta, 0.0), axis=1, keepdims=True)
        gate = jnp.sum(jnp.where(lane == ge + 64, meta, 0.0), axis=1, keepdims=True)
        sel[e] = jnp.where(lane == code.astype(jnp.int32) + base_col, 1.0, 0.0).astype(BF)
        gates[e] = jnp.broadcast_to(gate, (ntok, 128))
        code_t = meta_t[pl.ds(ge, 1), :].astype(jnp.int32) + base_row
        sel_t[pl.ds(e * rows, rows), :] = jnp.where(slot_row == code_t, 1.0, 0.0).astype(BF)

    fwd_y(2, 1)
    fwd_y(1, 1)
    fwd_y(3, 0)
    fwd_y(3, 1)
    for i in range(NA):
        for yy in range(2):
            for zz in range(4):
                arrive((1 - c, yy, zz), i)

    @pl.loop(0, hidden // 512)
    def _(n):
        cols = pl.ds(pl.multiple_of(n * 512, 512), 512)
        hh = h_all[:, :, :, :, cols].reshape(ntok, 512)
        xe[:, cols] = jnp.dot(sel_t[...], hh, preferred_element_type=F32).astype(BF)

    for e in range(num_loc):
        g_wait(2 * e)
        g_wait(2 * e + 1)

        def put(start, size, v, e=e):
            act[e, :, pl.ds(start, size)] = v
        gate_up(lambda e=e: xe[pl.ds(e * rows, rows), :], g_slot(2 * e), g_slot(2 * e + 1), put)
        if e == 0:
            g_copy(6).start()
            g_copy(7).start()
        elif e < 3:
            for p in range(4 * e + 4, 4 * e + 8):
                d_copy(p).start()
        else:
            g_copy(8).start()
            g_copy(9).start()

    def rdma(src, dst, send_sem, recv_sem, peer):
        return pltpu.make_async_remote_copy(src_ref=src, dst_ref=dst, send_sem=send_sem, recv_sem=recv_sem, device_id={"ep": peer}, device_id_type=MESH)

    def chunk(j):
        return pl.ds(j * cw, cw)

    def s1(j):
        return rdma(part.at[1 - c, :, :, :, chunk(j)], rc.at[:, :, :, chunk(j)], s1_send.at[j], s1_recv.at[j], core_peer)

    def s2(j):
        return rdma(part.at[c, 1 - y, :, :, chunk(j)], ry.at[:, :, chunk(j)], s2_send.at[j], s2_recv.at[j], y_peer)

    def s3(j, i):
        return rdma(part.at[c, y, (zc, za)[i], :, chunk(j)], rz.at[i, :, chunk(j)], s3_send.at[2 * j + i], s3_recv.at[2 * j + i], za_peer)

    def s4(j):
        return rdma(part.at[c, y, zb, :, chunk(j)], rz.at[2, :, chunk(j)], s4_send.at[j], s4_recv.at[j], zb_peer)

    def step_a(j):
        cols = chunk(j)
        s1(j).wait_recv()
        part[c, 1 - y, :, :, cols] = part[c, 1 - y, :, :, cols] + rc[1 - y, :, :, cols]
        s2(j).start()
        part[c, y, :, :, cols] = part[c, y, :, :, cols] + rc[y, :, :, cols]

    def step_b(j):
        cols = chunk(j)
        s2(j).wait_recv()
        part[c, y, :, :, cols] = part[c, y, :, :, cols] + ry[:, :, cols]
        s3(j, 0).start()
        s3(j, 1).start()

    def step_c(j):
        cols = chunk(j)
        s3(j, 0).wait_recv()
        part[c, y, zb, :, cols] = part[c, y, zb, :, cols] + rz[0, :, cols]
        s4(j).start()

    def step_f(j):
        cols = chunk(j)
        s3(j, 1).wait_recv()
        s4(j).wait_recv()
        routed = part[c, y, z, :, cols] + rz[1, :, cols] + rz[2, :, cols]
        out_ref[:, cols] = (h_own[:, cols].astype(F32) + shared[:, cols].astype(F32) + routed).astype(BF)

    def down(j):
        cols = chunk(j)
        if j % 2 == 0:
            for e in range(num_loc):
                d_copy(2 * j + e).wait()
        for e in range(num_loc):
            buf, at = d_place(j // 2 * 4 + e)
            o = jnp.dot(act[e], buf[at[0], at[1], pl.ds(j % 2 * cw + (j // 2 > 1) * (e % 2) * dw, cw)] if buf is gbuf else buf[at[0], :, pl.ds(j % 2 * cw, cw)], preferred_element_type=F32).astype(BF)
            b = jnp.dot(sel[e], o, preferred_element_type=F32)
            gt = gates[e]
            b = (b * jnp.concatenate([gt] * (cw // 128), axis=1)).reshape(2, 2, 4, num_seq, cw)
            if e == 0:
                part[:, :, :, :, cols] = b
            else:
                part[:, :, :, :, cols] = part[:, :, :, :, cols] + b
        if j in (1, 3):
            for e in range(num_loc):
                d_copy(16 + 2 * (j - 1) + e).start()
        if j == 5:
            g_copy(10).start()
            g_copy(11).start()

    def shared_up(i):
        s, b = i // 3, i % 3
        if b == 0:
            g_wait(8 + 2 * s)
            g_wait(9 + 2 * s)

        def put(start, size, v):
            act_sh[s, :, pl.ds(start, size)] = v
        gate_up(lambda: h_own[...], g_slot(8 + 2 * s), g_slot(9 + 2 * s), put, (512 * b,))

    def shared_down(i):
        d_copy(16 + 2 * i).wait()
        d_copy(17 + 2 * i).wait()
        o = jnp.dot(act_sh[0], dbuf[2 * i], preferred_element_type=F32) + jnp.dot(act_sh[1], dbuf[2 * i + 1], preferred_element_type=F32)
        shared[:, i * dw:(i + 1) * dw] = o.astype(BF)

    for j in range(NCH):
        down(j)
        s1(j).start()
        if j >= 1:
            step_a(j - 1)
        if j == 6:
            step_b(0)
    step_a(NCH - 1)
    fill = [lambda i=i: shared_up(i) for i in range(6)] + [lambda i=i: shared_down(i) for i in range(4)]
    plan = [1, 2, 2, 2, 1, 1, 1]
    for j in range(1, NCH):
        step_b(j)
        for _ in range(plan[j - 1]):
            fill.pop(0)()
        step_c(j - 1)
        if j == NCH - 1:
            for i in range(NCH - 1):
                step_f(i)
    step_c(NCH - 1)
    step_f(NCH - 1)
    for a in started:
        a.wait_send()
    for j in range(NCH):
        s1(j).wait_send()
        s2(j).wait_send()
        s3(j, 0).wait_send()
        s3(j, 1).wait_send()
        s4(j).wait_send()


def layer(x, lens, routes, route_gates, cache, w_q, w_dkv, w_uk, w_uv, w_o, sh_gate, sh_up, sh_down, ex_gate, ex_up, ex_down):
    num_seq, hidden = x.shape
    num_loc, _, ff = ex_gate.shape
    lat_row = cache.shape[1]
    ntok = 16 * num_seq
    dma = pltpu.SemaphoreType.DMA
    vm = pl.BlockSpec(memory_space=pltpu.VMEM)
    hbm = pl.BlockSpec(memory_space=pl.ANY)
    return pl.pallas_call(
        layer_kernel,
        out_shape=(jax.ShapeDtypeStruct((num_seq, hidden), BF), jax.ShapeDtypeStruct((num_seq, lat_row), BF)),
        in_specs=[vm] * 4 + [hbm] * 12,
        out_specs=(vm, vm),
        scratch_shapes=[
            pltpu.VMEM((NG, hidden, ff), BF),
            pltpu.VMEM((ND, ff, 2 * hidden // NCH), BF),
            pltpu.VMEM((16, num_seq, 128), BF),
            pltpu.VMEM((num_seq, 640), F32),
            pltpu.VMEM((num_seq, 128), F32),
            pltpu.VMEM((num_seq, hidden), BF),
            pltpu.VMEM((num_seq, hidden), BF),
            pltpu.VMEM((num_seq, 128), F32),
            pltpu.VMEM((2, 2, 4, num_seq, hidden), BF),
            pltpu.VMEM((2, 2, 4, num_seq, 128), F32),
            pltpu.VMEM((128, ntok), F32),
            pltpu.VMEM((num_loc, ntok, 128), BF),
            pltpu.VMEM((num_loc * 128, ntok), BF),
            pltpu.VMEM((num_loc, ntok, 128), F32),
            pltpu.VMEM((num_loc * 128, hidden), BF),
            pltpu.VMEM((num_loc, 128, ff), BF),
            pltpu.VMEM((2, num_seq, ff), BF),
            pltpu.VMEM((num_seq, hidden), BF),
            pltpu.VMEM((2, 2, 4, num_seq, hidden), F32),
            pltpu.VMEM((2, 4, num_seq, hidden), F32),
            pltpu.VMEM((4, num_seq, hidden), F32),
            pltpu.VMEM((3, num_seq, hidden), F32),
            dma((NG,)), dma((16,)), dma((num_seq,)), dma((7,)), dma((15 * NA,)), dma((16 * NA,)), dma((15,)), dma((16,)),
            dma((NCH,)), dma((NCH,)), dma((NCH,)), dma((NCH,)), dma((2 * NCH,)), dma((2 * NCH,)), dma((NCH,)), dma((NCH,)),
        ],
        compiler_params=pltpu.CompilerParams(collective_id=0, has_side_effects=True, vmem_limit_bytes=67043328),
        name="layer",
    )(x, lens, routes, route_gates, cache, w_q, w_dkv, w_uk, w_uv, w_o, sh_gate, sh_up, sh_down, ex_gate, ex_up, ex_down)


def solution(mesh):
    def device_step(x_blk, cache_blk, len_blk, routes, route_gates, w_q, w_dkv, w_uk, w_uv, w_o, sh_gate, sh_up, sh_down, ex_gate, ex_up, ex_down):
        lens = len_blk[None, :]
        uk = w_uk.reshape(-1, w_uk.shape[2])
        uv = w_uv.reshape(-1, w_uv.shape[2])
        return layer(x_blk, lens, routes.T, route_gates.T, cache_blk.transpose(0, 2, 1), w_q, w_dkv.T, uk, uv, w_o, sh_gate, sh_up, sh_down, ex_gate, ex_up, ex_down)

    batch_spec = P(("dp", "ep"))
    weight_spec = P()
    expert_spec = P("ep")
    in_specs = (batch_spec,) * 5 + (weight_spec,) * 8 + (expert_spec,) * 3
    return jax.shard_map(device_step, mesh=mesh, in_specs=in_specs, out_specs=(batch_spec, batch_spec), check_vma=False)
```

```python
import functools

import jax
import jax.numpy as jnp
from jax import lax
from jax.experimental import pallas as pl
from jax.experimental.pallas import tpu as pltpu
from jax.sharding import PartitionSpec as P

MESH = pl.DeviceIdType.MESH
BF = jnp.bfloat16
F32 = jnp.float32


LN = 128
NG = 6
ND = 8
NCH = 8
NA = 2
ZYC = (2, 2, 4)
YLAST = (0, 2)


def layer_kernel(x_ref, len_ref, routes_ref, rgate_ref, cache_ref, wq_ref, wdkv_ref, wuk_ref, wuv_ref, wo_ref,
                 sg_ref, su_ref, sd_ref, eg_ref, eu_ref, ed_ref, out_ref, kv_ref,
                 gbuf, dbuf, qn, kvf, lenb, vcat, h_own, meta_own,
                 h_all, meta_all, meta_t, sel, sel_t, gates, xe, act, act_sh, shared,
                 part, rc, ry, rz,
                 gsem, dsem, csem, xsem, ag_send, ag_recv, am_send, am_recv,
                 s1_send, s1_recv, s2_send, s2_recv, s3_send, s3_recv, s4_send, s4_recv):
    me = lax.axis_index("ep")
    c = lax.rem(me, 2)
    y = lax.rem(lax.div(me, 2), 2)
    z = lax.div(me, 4)
    core_peer = me + 1 - 2 * c
    y_peer = me + 2 - 4 * y
    za = z + 1 - 2 * lax.rem(z, 2)
    zb = z + 2 - 4 * lax.div(z, 2)
    zc = za + zb - z
    za_peer = me + 4 * (za - z)
    zb_peer = me + 4 * (zb - z)
    num_loc, hidden, ff = eg_ref.shape
    num_seq = x_ref.shape[0]
    cw = hidden // NCH
    dw = 2 * cw
    aw = hidden // NA
    latent = wuk_ref.shape[1]
    num_heads = part.shape[0] * part.shape[1] * part.shape[2]
    nope = wuk_ref.shape[0] // num_heads
    rope = wdkv_ref.shape[0] - latent
    qw = nope + rope
    top_k = routes_ref.shape[0]
    lat_row, cache_len = cache_ref.shape[1:]

    W6 = 6 * qw
    W4 = 4 * qw
    OB = hidden - ff

    def a_copy(k):
        if k < 2:
            src, dst = wq_ref.at[:, pl.ds(k * W6, W6)], gbuf.at[k, :, pl.ds(0, W6)]
        elif k == 2:
            src, dst = wq_ref.at[:, pl.ds(2 * W6, W4)], gbuf.at[k, :, pl.ds(0, W4)]
        elif k == 3:
            src, dst = wo_ref.at[:, pl.ds(ff, OB)], gbuf.at[k, :, pl.ds(0, OB)]
        else:
            src, dst = wo_ref.at[:, pl.ds(0, ff)], gbuf.at[k]
        return pltpu.make_async_copy(src, dst, gsem.at[k])

    def g_slot(m):
        return m % NG if m < 8 else m - 8

    def g_copy(m):
        if m < 8:
            src = (eg_ref, eu_ref)[m % 2].at[m // 2]
        else:
            src = (sg_ref, su_ref)[m % 2].at[:, pl.ds((m - 8) // 2 * ff, ff)]
        return pltpu.make_async_copy(src, gbuf.at[g_slot(m)], gsem.at[g_slot(m)])

    def uk_copy():
        return pltpu.make_async_copy(wuk_ref, gbuf.at[2, :, pl.ds(W4, latent)], xsem.at[0])

    def uv_copy(i):
        return pltpu.make_async_copy(wuv_ref.at[pl.ds(i * hidden, hidden)], gbuf.at[3, :, pl.ds(OB + LN * i, LN)], xsem.at[1 + i])

    def dkv_copy(i):
        lo, size = ((0, ff), (ff, OB))[i]
        return pltpu.make_async_copy(wdkv_ref.at[:, pl.ds(lo, size)], gbuf.at[5, pl.ds(i * lat_row, lat_row), pl.ds(0, size)], xsem.at[5 + i])

    def cache_at(i, slot):
        return slot, pl.ds(i % 4 // 2 * lat_row, lat_row), pl.ds(i % 2 * cache_len, cache_len)

    def c_copy(i, seq, slot):
        return pltpu.make_async_copy(cache_ref.at[seq], dbuf.at[cache_at(i, slot)], csem.at[seq])

    def d_place(p):
        if 8 <= p < 16:
            return gbuf, (2 + (p - 8) // 2, pl.ds(0, ff), pl.ds(p % 2 * dw, dw))
        return dbuf, (p % ND, slice(None), slice(None))

    def d_copy(p):
        if p < 16:
            src = ed_ref.at[p % 4, :, pl.ds((p // 4) * dw, dw)]
        else:
            q = p - 16
            src = sd_ref.at[pl.ds((q % 2) * ff, ff), pl.ds((q // 2) * dw, dw)]
        buf, at = d_place(p)
        return pltpu.make_async_copy(src, buf.at[at], dsem.at[p % 16])

    for k in range(3):
        a_copy(k).start()
    uk_copy().start()
    dkv_copy(0).start()
    dkv_copy(1).start()
    for i in range(num_seq):
        c_copy(i, i, i // 4).start()
    a_copy(3).start()
    for i in range(4):
        uv_copy(i).start()
    a_copy(4).start()

    barrier = pltpu.get_barrier_semaphore()
    peers = [core_peer, y_peer, za_peer, zb_peer]
    for peer in peers:
        pl.semaphore_signal(barrier, inc=1, device_id={"ep": peer}, device_id_type=MESH)

    lane = lax.broadcasted_iota(jnp.int32, (num_seq, LN), 1)
    pad_k = jnp.zeros((8 - top_k, num_seq), F32)
    small = jnp.concatenate([routes_ref[...].astype(F32), pad_k, rgate_ref[...], pad_k, len_ref[...].astype(F32), jnp.zeros((15, num_seq), F32)], axis=0)
    small = jnp.concatenate([small, jnp.zeros((32, LN - num_seq), F32)], axis=1)
    cols = jnp.concatenate([small, jnp.zeros((96, LN), F32)], axis=0).T[:num_seq]
    lenb[...] = jnp.broadcast_to(cols[:, 16:17], (num_seq, LN))
    member = jnp.zeros((num_seq, LN), F32)
    gate_te = jnp.zeros((num_seq, LN), F32)
    for k in range(top_k):
        hit = (lane % 64).astype(F32) == cols[:, k:k + 1]
        member = jnp.where(hit, 1.0, member)
        gate_te = jnp.where(hit, cols[:, 8 + k:9 + k], gate_te)
    tri = jnp.where(lax.broadcasted_iota(jnp.int32, (num_seq, num_seq), 0) > lax.broadcasted_iota(jnp.int32, (num_seq, num_seq), 1), 1.0, 0.0)
    rank = jnp.dot(tri.astype(BF), member.astype(BF), preferred_element_type=F32)
    meta_own[...] = jnp.where(lane < 64, jnp.where(member > 0.5, rank, -4096.0), gate_te)

    freq = jnp.exp((lane % (rope // 2)).astype(F32) * (-2.0 * 9.210340371976184 / rope))
    angle = lenb[...] * freq
    live = lane < rope
    cos_w = jnp.where(live, jnp.cos(angle), 0.0)
    sin_w = jnp.where(live, jnp.where(lane < rope // 2, -jnp.sin(angle), jnp.sin(angle)), 0.0)

    def rotate(v):
        turned = jnp.where(lane < rope // 2, pltpu.roll(v, LN - rope // 2, 1), pltpu.roll(v, rope // 2, 1))
        return v * cos_w + turned * sin_w

    def ag(src_pos, peer, n, own, part_no):
        cc, yy, zz = src_pos
        idx = (cc * 2 + yy) * 4 + zz
        if part_no is None:
            src = meta_own if own else meta_all.at[cc, yy, zz]
            return pltpu.make_async_remote_copy(src_ref=src, dst_ref=meta_all.at[cc, yy, zz], send_sem=am_send.at[n], recv_sem=am_recv.at[idx], device_id={"ep": peer}, device_id_type=MESH)
        cols = pl.ds(part_no * aw, aw)
        src = h_own.at[:, cols] if own else h_all.at[cc, yy, zz, :, cols]
        return pltpu.make_async_remote_copy(src_ref=src, dst_ref=h_all.at[cc, yy, zz, :, cols], send_sem=ag_send.at[part_no * 15 + n], recv_sem=ag_recv.at[part_no * 16 + idx], device_id={"ep": peer}, device_id_type=MESH)

    started = []

    def send(src_pos, peer, n, part_no, own=False):
        a = ag(src_pos, peer, n, own, part_no)
        a.start()
        started.append(a)

    def arrive(src_pos, part_no):
        ag(src_pos, core_peer, 0, False, part_no).wait_recv()

    def send_own(part_no):
        for n, peer in enumerate((zb_peer, y_peer, za_peer, core_peer)):
            send((c, y, z), peer, n, part_no, True)

    def fwd_zb(part_no):
        pos = (c, y, zb)
        arrive(pos, part_no)
        send(pos, za_peer, 4, part_no)
        send(pos, y_peer, 5, part_no)
        send(pos, core_peer, 6, part_no)

    def fwd_za(part_no):
        pos = (c, y, za)
        arrive(pos, part_no)
        send(pos, y_peer, 7, part_no)
        send(pos, core_peer, 8, part_no)

    def fwd_zc(part_no):
        pos = (c, y, zc)
        arrive(pos, part_no)
        send(pos, y_peer, 9, part_no)
        send(pos, core_peer, 10, part_no)

    def fwd_y(i, part_no):
        pos = (c, 1 - y, (z, zb, za, zc)[i])
        arrive(pos, part_no)
        send(pos, core_peer, 11 + i, part_no)

    def hidx(h):
        return h // 8, h // 4 % 2, h % 4

    def q_heads(k, first, count):
        a_copy(k).wait()
        qq = jnp.dot(x_ref[...], gbuf[k, :, pl.ds(0, count * qw)], preferred_element_type=F32).astype(BF).astype(F32)
        for i in range(count // 2):
            pair = qq[:, 2 * i * qw:2 * (i + 1) * qw]
            for h, v in ((first + 2 * i, pair), (first + 2 * i + 1, pltpu.roll(pair, qw, 1))):
                qn[h] = v[:, :nope].astype(BF)
                part[(*hidx(h), slice(None), pl.ds(latent, LN))] = rotate(v[:, nope:nope + LN])

    q_heads(0, 0, 6)
    g_copy(0).start()
    q_heads(1, 6, 6)
    g_copy(1).start()
    q_heads(2, 12, 4)
    uk_copy().wait()
    for h in range(num_heads):
        part[(*hidx(h), slice(None), pl.ds(0, latent))] = jnp.dot(qn[h], gbuf[2, pl.ds(h * nope, nope), pl.ds(W4, latent)], preferred_element_type=F32)
    g_copy(2).start()
    pl.semaphore_wait(barrier, len(peers))
    send_own(None)
    meta_all[c, y, z] = meta_own[...]

    nt = (((1,), (1,)), ((), ()))
    dkv_copy(0).wait()
    dkv_copy(1).wait()
    r = lax.dot_general(x_ref[:, :ff], gbuf[5, pl.ds(0, lat_row), :], nt, preferred_element_type=F32) + lax.dot_general(x_ref[:, ff:], gbuf[5, pl.ds(lat_row, lat_row), pl.ds(0, OB)], nt, preferred_element_type=F32)
    g_copy(5).start()
    r_lat = r[:, :latent].astype(BF)
    r_rope = rotate(jnp.concatenate([r[:, latent:], jnp.zeros((num_seq, LN - rope), F32)], axis=1)).astype(BF)
    kvf[:, :latent] = r_lat.astype(F32)
    kvf[:, latent:] = r_rope.astype(F32)
    kv_ref[:, :latent] = r_lat
    kv_ref[:, latent:] = r_rope[:, :rope]

    scale = qw ** -0.5

    @pl.loop(0, num_seq // 8)
    def _(g):
        for b in range(8):
            c_copy(b, g * 8 + b, 2 * g + b // 4).wait()
        rows8 = pl.ds(pl.multiple_of(g * 8, 8), 8)
        q = part[:, :, :, rows8, pl.ds(0, latent + LN)].reshape(LN, latent + LN).astype(BF)
        kv_rep = jnp.broadcast_to(kvf[rows8, :][None], (16, 8, latent + LN)).reshape(LN, latent + LN)
        n_rep = jnp.broadcast_to(lenb[rows8, :][None], (16, 8, LN)).reshape(LN, LN)
        n_rep = jnp.concatenate([n_rep, n_rep], axis=1)
        row = lax.broadcasted_iota(jnp.int32, (LN, 256), 0) % 8
        pos = lax.broadcasted_iota(jnp.int32, (LN, 256), 1).astype(F32)
        s_new = jnp.sum(q.astype(F32) * kv_rep, axis=1, keepdims=True) * scale
        q = q[:, :latent + rope]
        s = jnp.zeros((LN, 256), F32)
        for b in range(8):
            s = jnp.where(row == b, jnp.dot(q, dbuf[cache_at(b, 2 * g + b // 4)], preferred_element_type=F32), s)
        s = jnp.where(pos < n_rep, s * scale, -jnp.inf)
        top = jnp.maximum(jnp.max(s, axis=1, keepdims=True), s_new)
        e = jnp.exp(s - top)
        e_new = jnp.exp(s_new - top)
        den = jnp.sum(e, axis=1, keepdims=True) + e_new
        p = e / den
        o = (e_new / den).astype(BF).astype(F32) * kv_rep[:, :latent]
        for b in range(8):
            o = o + lax.dot_general(jnp.where(row == b, p, 0.0).astype(BF), dbuf[cache_at(b, 2 * g + b // 4)][:latent], nt, preferred_element_type=F32)
        part[:, :, :, rows8, pl.ds(1024, latent)] = o.reshape(*ZYC, 8, latent)

    for p in range(ND):
        d_copy(p).start()
    fwd_zb(None)
    fwd_za(None)
    for i in range(4):
        uv_copy(i).wait()
    a_copy(3).wait()
    for h in range(num_heads):
        ob = part[(*hidx(h), slice(None), pl.ds(1024, latent))].astype(BF)
        vcat[:, h * LN:(h + 1) * LN] = jnp.dot(ob, gbuf[3, pl.ds(h % 4 * latent, latent), pl.ds(OB + LN * (h // 4), LN)], preferred_element_type=F32).astype(BF)
    a_copy(4).wait()
    fwd_zc(None)
    for lo, hi, slot in ((0, ff, 4), (ff, hidden, 3)):
        a = jnp.dot(vcat[...], gbuf[slot, :, pl.ds(0, hi - lo)], preferred_element_type=F32).astype(BF)
        h_own[:, lo:hi] = (x_ref[:, lo:hi].astype(F32) + a.astype(F32)).astype(BF)
        for i in range(NA):
            if lo < (i + 1) * aw <= hi:
                send_own(i)
    g_copy(3).start()
    g_copy(4).start()
    h_all[c, y, z] = h_own[...]
    for i in range(4):
        fwd_y(i, None)
    fwd_za(0)
    fwd_zb(0)
    fwd_y(0, 0)
    fwd_za(1)
    fwd_zb(1)
    fwd_zc(0)
    fwd_y(0, 1)
    fwd_y(2, 0)
    fwd_y(1, 0)
    fwd_zc(1)

    def gate_up(x, gslot, uslot, store, starts=None):
        for start in starts or range(0, ff, 512):
            size = min(512, ff - start)
            g = jnp.dot(x(), gbuf[gslot, :, pl.ds(start, size)], preferred_element_type=F32)
            u = jnp.dot(x(), gbuf[uslot, :, pl.ds(start, size)], preferred_element_type=F32)
            store(start, size, (g * jax.nn.sigmoid(g) * u).astype(BF))

    def g_wait(k):
        g_copy(k).wait()

    for yy in range(2):
        for zz in range(4):
            arrive((1 - c, yy, zz), None)

    ntok = 16 * num_seq
    rows = 16 * 8
    meta = meta_all[...].reshape(ntok, LN)
    meta_t[...] = meta.T
    lane = lax.broadcasted_iota(jnp.int32, (ntok, LN), 1)
    base_col = lax.broadcasted_iota(jnp.int32, (ntok, LN), 0) // num_seq * 8
    base_row = lax.broadcasted_iota(jnp.int32, (1, ntok), 1) // num_seq * 8
    slot_row = lax.broadcasted_iota(jnp.int32, (rows, ntok), 0)
    for e in range(num_loc):
        ge = me * num_loc + e
        code = jnp.sum(jnp.where(lane == ge, meta, 0.0), axis=1, keepdims=True)
        gate = jnp.sum(jnp.where(lane == ge + 64, meta, 0.0), axis=1, keepdims=True)
        sel[e] = jnp.where(lane == code.astype(jnp.int32) + base_col, 1.0, 0.0).astype(BF)
        gates[e] = jnp.broadcast_to(gate, (ntok, LN))
        code_t = meta_t[pl.ds(ge, 1), :].astype(jnp.int32) + base_row
        sel_t[pl.ds(e * rows, rows), :] = jnp.where(slot_row == code_t, 1.0, 0.0).astype(BF)

    fwd_y(2, 1)
    fwd_y(1, 1)
    fwd_y(3, 0)
    fwd_y(3, 1)
    for i in range(NA):
        for yy in range(2):
            for zz in range(4):
                arrive((1 - c, yy, zz), i)

    @pl.loop(0, hidden // 512)
    def _(n):
        cols = pl.ds(pl.multiple_of(n * 512, 512), 512)
        hh = h_all[:, :, :, :, cols].reshape(ntok, 512)
        xe[:, cols] = jnp.dot(sel_t[...], hh, preferred_element_type=F32).astype(BF)

    for e in range(num_loc):
        g_wait(2 * e)
        g_wait(2 * e + 1)

        def put(start, size, v, e=e):
            act[e, :, pl.ds(start, size)] = v
        gate_up(lambda e=e: xe[pl.ds(e * rows, rows), :], g_slot(2 * e), g_slot(2 * e + 1), put)
        if e == 0:
            g_copy(6).start()
            g_copy(7).start()
        elif e < 3:
            for p in range(4 * e + 4, 4 * e + 8):
                d_copy(p).start()
        else:
            g_copy(8).start()
            g_copy(9).start()

    def rdma(src, dst, send_sem, recv_sem, peer):
        return pltpu.make_async_remote_copy(src_ref=src, dst_ref=dst, send_sem=send_sem, recv_sem=recv_sem, device_id={"ep": peer}, device_id_type=MESH)

    def chunk(j):
        return pl.ds(j * cw, cw)

    def s1(j):
        return rdma(part.at[1 - c, :, :, :, chunk(j)], rc.at[:, :, :, chunk(j)], s1_send.at[j], s1_recv.at[j], core_peer)

    def s2(j):
        return rdma(part.at[c, 1 - y, :, :, chunk(j)], ry.at[:, :, chunk(j)], s2_send.at[j], s2_recv.at[j], y_peer)

    def s3(j, i):
        return rdma(part.at[c, y, (zc, za)[i], :, chunk(j)], rz.at[i, :, chunk(j)], s3_send.at[2 * j + i], s3_recv.at[2 * j + i], za_peer)

    def s4(j):
        return rdma(part.at[c, y, zb, :, chunk(j)], rz.at[2, :, chunk(j)], s4_send.at[j], s4_recv.at[j], zb_peer)

    def step_a(j):
        cols = chunk(j)
        s1(j).wait_recv()
        part[c, 1 - y, :, :, cols] = part[c, 1 - y, :, :, cols] + rc[1 - y, :, :, cols]
        s2(j).start()
        part[c, y, :, :, cols] = part[c, y, :, :, cols] + rc[y, :, :, cols]

    def step_b(j):
        cols = chunk(j)
        s2(j).wait_recv()
        part[c, y, :, :, cols] = part[c, y, :, :, cols] + ry[:, :, cols]
        s3(j, 0).start()
        s3(j, 1).start()

    def step_c(j):
        cols = chunk(j)
        s3(j, 0).wait_recv()
        part[c, y, zb, :, cols] = part[c, y, zb, :, cols] + rz[0, :, cols]
        s4(j).start()

    def t3(j, i):
        return rdma(part.at[c, :, (zc, za)[i], :, chunk(j)], ry.at[pl.ds(2 * i, 2), :, chunk(j)], s3_send.at[2 * j + i], s3_recv.at[2 * j + i], za_peer)

    def t4(j):
        return rdma(part.at[c, :, zb, :, chunk(j)], rz.at[pl.ds(0, 2), :, chunk(j)], s4_send.at[j], s4_recv.at[j], zb_peer)

    def t2(j):
        return rdma(part.at[c, 1 - y, z, :, chunk(j)], rz.at[2, :, chunk(j)], s2_send.at[j], s2_recv.at[j], y_peer)

    def turn_a(j):
        cols = chunk(j)
        s1(j).wait_recv()
        part[c, :, :, :, cols] = part[c, :, :, :, cols] + rc[:, :, :, cols]
        t3(j, 0).start()
        t3(j, 1).start()

    def turn_b(j):
        cols = chunk(j)
        t3(j, 0).wait_recv()
        part[c, :, zb, :, cols] = part[c, :, zb, :, cols] + ry[0:2, :, cols]
        t4(j).start()

    def turn_c(j):
        cols = chunk(j)
        t3(j, 1).wait_recv()
        t4(j).wait_recv()
        part[c, :, z, :, cols] = part[c, :, z, :, cols] + ry[2:4, :, cols] + rz[0:2, :, cols]
        t2(j).start()

    def step_f(j):
        cols = chunk(j)
        if j in YLAST:
            t2(j).wait_recv()
            routed = part[c, y, z, :, cols] + rz[2, :, cols]
        else:
            s3(j, 1).wait_recv()
            s4(j).wait_recv()
            routed = part[c, y, z, :, cols] + rz[1, :, cols] + rz[2, :, cols]
        out_ref[:, cols] = (h_own[:, cols].astype(F32) + shared[:, cols].astype(F32) + routed).astype(BF)

    def down(j):
        cols = chunk(j)
        if j % 2 == 0:
            for e in range(num_loc):
                d_copy(2 * j + e).wait()
        for e in range(num_loc):
            buf, at = d_place(j // 2 * 4 + e)
            o = jnp.dot(act[e], buf[at[0], at[1], pl.ds(j % 2 * cw + (j // 2 > 1) * (e % 2) * dw, cw)] if buf is gbuf else buf[at[0], :, pl.ds(j % 2 * cw, cw)], preferred_element_type=F32).astype(BF)
            b = jnp.dot(sel[e], o, preferred_element_type=F32)
            gt = gates[e]
            b = (b * jnp.concatenate([gt] * (cw // LN), axis=1)).reshape(*ZYC, num_seq, cw)
            if e == 0:
                part[:, :, :, :, cols] = b
            else:
                part[:, :, :, :, cols] = part[:, :, :, :, cols] + b
        if j in (1, 3):
            for e in range(num_loc):
                d_copy(16 + 2 * (j - 1) + e).start()
        if j == 5:
            g_copy(10).start()
            g_copy(11).start()

    def shared_up(i):
        s, b = i // 3, i % 3
        if b == 0:
            g_wait(8 + 2 * s)
            g_wait(9 + 2 * s)

        def put(start, size, v):
            act_sh[s, :, pl.ds(start, size)] = v
        gate_up(lambda: h_own[...], g_slot(8 + 2 * s), g_slot(9 + 2 * s), put, (512 * b,))

    def shared_down(i):
        d_copy(16 + 2 * i).wait()
        d_copy(17 + 2 * i).wait()
        o = jnp.dot(act_sh[0], dbuf[2 * i], preferred_element_type=F32) + jnp.dot(act_sh[1], dbuf[2 * i + 1], preferred_element_type=F32)
        shared[:, i * dw:(i + 1) * dw] = o.astype(BF)

    fill = [lambda i=i: shared_up(i) for i in range(6)] + [lambda i=i: shared_down(i) for i in range(4)]

    def work(n):
        for _ in range(n):
            fill.pop(0)()

    def enter(j):
        (turn_a if j in YLAST else step_a)(j)

    for j in range(NCH):
        down(j)
        s1(j).start()
        if j >= 1:
            enter(j - 1)
        if j == 5:
            turn_b(0)
        if j == 6:
            step_b(1)
    enter(7)
    turn_b(2)
    step_b(3)
    step_c(1)
    work(1)
    turn_c(0)
    step_b(4)
    step_c(3)
    work(1)
    step_b(5)
    step_c(4)
    work(1)
    turn_c(2)
    step_b(6)
    step_c(5)
    work(1)
    step_b(7)
    step_c(6)
    work(3)
    step_c(7)
    work(3)
    for j in range(NCH):
        step_f(j)
    for a in started:
        a.wait_send()
    for j in range(NCH):
        s1(j).wait_send()
        if j in YLAST:
            copies = (t2(j), t3(j, 0), t3(j, 1), t4(j))
        else:
            copies = (s2(j), s3(j, 0), s3(j, 1), s4(j))
        for a in copies:
            a.wait_send()


def layer(x, lens, routes, route_gates, cache, w_q, w_dkv, w_uk, w_uv, w_o, sh_gate, sh_up, sh_down, ex_gate, ex_up, ex_down):
    num_seq, hidden = x.shape
    num_loc, _, ff = ex_gate.shape
    lat_row = cache.shape[1]
    ntok = 16 * num_seq
    dma = pltpu.SemaphoreType.DMA
    vm = pl.BlockSpec(memory_space=pltpu.VMEM)
    hbm = pl.BlockSpec(memory_space=pl.ANY)
    return pl.pallas_call(
        layer_kernel,
        out_shape=(jax.ShapeDtypeStruct((num_seq, hidden), BF), jax.ShapeDtypeStruct((num_seq, lat_row), BF)),
        in_specs=[vm] * 4 + [hbm] * 12,
        out_specs=(vm, vm),
        scratch_shapes=[
            pltpu.VMEM((NG, hidden, ff), BF),
            pltpu.VMEM((ND, ff, 2 * hidden // NCH), BF),
            pltpu.VMEM((16, num_seq, LN), BF),
            pltpu.VMEM((num_seq, 640), F32),
            pltpu.VMEM((num_seq, LN), F32),
            pltpu.VMEM((num_seq, hidden), BF),
            pltpu.VMEM((num_seq, hidden), BF),
            pltpu.VMEM((num_seq, LN), F32),
            pltpu.VMEM((*ZYC, num_seq, hidden), BF),
            pltpu.VMEM((*ZYC, num_seq, LN), F32),
            pltpu.VMEM((LN, ntok), F32),
            pltpu.VMEM((num_loc, ntok, LN), BF),
            pltpu.VMEM((num_loc * LN, ntok), BF),
            pltpu.VMEM((num_loc, ntok, LN), F32),
            pltpu.VMEM((num_loc * LN, hidden), BF),
            pltpu.VMEM((num_loc, LN, ff), BF),
            pltpu.VMEM((2, num_seq, ff), BF),
            pltpu.VMEM((num_seq, hidden), BF),
            pltpu.VMEM((*ZYC, num_seq, hidden), F32),
            pltpu.VMEM((2, 4, num_seq, hidden), F32),
            pltpu.VMEM((4, num_seq, hidden), F32),
            pltpu.VMEM((3, num_seq, hidden), F32),
            dma((NG,)), dma((16,)), dma((num_seq,)), dma((7,)), dma((15 * NA,)), dma((16 * NA,)), dma((15,)), dma((16,)),
            dma((NCH,)), dma((NCH,)), dma((NCH,)), dma((NCH,)), dma((2 * NCH,)), dma((2 * NCH,)), dma((NCH,)), dma((NCH,)),
        ],
        compiler_params=pltpu.CompilerParams(collective_id=0, has_side_effects=True, vmem_limit_bytes=67043328),
        name="layer",
    )(x, lens, routes, route_gates, cache, w_q, w_dkv, w_uk, w_uv, w_o, sh_gate, sh_up, sh_down, ex_gate, ex_up, ex_down)


def finish_kernel(a_ref, b_ref, c_ref, d_ref):
    c_ref[...] = a_ref[...]
    d_ref[...] = b_ref[...]


def finish(a, b):
    vm = pl.BlockSpec(memory_space=pltpu.VMEM)
    return pl.pallas_call(finish_kernel, out_shape=(jax.ShapeDtypeStruct(a.shape, a.dtype), jax.ShapeDtypeStruct(b.shape, b.dtype)), in_specs=[vm, vm], out_specs=(vm, vm), name="finish")(a, b)


def solution(mesh):
    def device_step(x_blk, cache_blk, len_blk, routes, route_gates, w_q, w_dkv, w_uk, w_uv, w_o, sh_gate, sh_up, sh_down, ex_gate, ex_up, ex_down):
        lens = len_blk[None, :]
        uk = w_uk.reshape(-1, w_uk.shape[2])
        uv = w_uv.reshape(-1, w_uv.shape[2])
        return finish(*layer(x_blk, lens, routes.T, route_gates.T, cache_blk.transpose(0, 2, 1), w_q, w_dkv.T, uk, uv, w_o, sh_gate, sh_up, sh_down, ex_gate, ex_up, ex_down))

    batch_spec = P(("dp", "ep"))
    weight_spec = P()
    expert_spec = P("ep")
    in_specs = (batch_spec,) * 5 + (weight_spec,) * 8 + (expert_spec,) * 3
    return jax.shard_map(device_step, mesh=mesh, in_specs=in_specs, out_specs=(batch_spec, batch_spec), check_vma=False)
```

```python
import functools

import jax
import jax.numpy as jnp
from jax import lax
from jax.experimental import pallas as pl
from jax.experimental.pallas import tpu as pltpu
from jax.sharding import PartitionSpec as P

MESH = pl.DeviceIdType.MESH
BF = jnp.bfloat16
F32 = jnp.float32


LN = 128
NG = 6
ND = 8
NCH = 8
NA = 2
ZYC = (2, 2, 4)
YLAST = (0, 1)


def layer_kernel(x_ref, len_ref, routes_ref, rgate_ref, cache_ref, wq_ref, wdkv_ref, wuk_ref, wuv_ref, wo_ref,
                 sg_ref, su_ref, sd_ref, eg_ref, eu_ref, ed_ref, out_ref, kv_ref,
                 gbuf, dbuf, qn, kvf, lenb, vcat, h_own, meta_own,
                 h_all, meta_all, meta_t, sel, sel_t, gates, xe, act, act_sh, shared,
                 part, rc, ry, rz,
                 gsem, dsem, csem, xsem, ag_send, ag_recv, am_send, am_recv,
                 s1_send, s1_recv, s2_send, s2_recv, s3_send, s3_recv, s4_send, s4_recv):
    me = lax.axis_index("ep")
    c = lax.rem(me, 2)
    y = lax.rem(lax.div(me, 2), 2)
    z = lax.div(me, 4)
    core_peer = me + 1 - 2 * c
    y_peer = me + 2 - 4 * y
    za = z + 1 - 2 * lax.rem(z, 2)
    zb = z + 2 - 4 * lax.div(z, 2)
    zc = za + zb - z
    za_peer = me + 4 * (za - z)
    zb_peer = me + 4 * (zb - z)
    num_loc, hidden, ff = eg_ref.shape
    num_seq = x_ref.shape[0]
    cw = hidden // NCH
    dw = 2 * cw
    aw = hidden // NA
    latent = wuk_ref.shape[1]
    num_heads = part.shape[0] * part.shape[1] * part.shape[2]
    nope = wuk_ref.shape[0] // num_heads
    rope = wdkv_ref.shape[0] - latent
    qw = nope + rope
    top_k = routes_ref.shape[0]
    lat_row, cache_len = cache_ref.shape[1:]

    W6 = 6 * qw
    W4 = 4 * qw
    OB = hidden - ff

    def a_copy(k):
        if k < 2:
            src, dst = wq_ref.at[:, pl.ds(k * W6, W6)], gbuf.at[k, :, pl.ds(0, W6)]
        elif k == 2:
            src, dst = wq_ref.at[:, pl.ds(2 * W6, W4)], gbuf.at[k, :, pl.ds(0, W4)]
        elif k == 3:
            src, dst = wo_ref.at[:, pl.ds(ff, OB)], gbuf.at[k, :, pl.ds(0, OB)]
        else:
            src, dst = wo_ref.at[:, pl.ds(0, ff)], gbuf.at[k]
        return pltpu.make_async_copy(src, dst, gsem.at[k])

    def g_slot(m):
        return m % NG if m < 8 else m - 8

    def g_copy(m):
        if m < 8:
            src = (eg_ref, eu_ref)[m % 2].at[m // 2]
        else:
            src = (sg_ref, su_ref)[m % 2].at[:, pl.ds((m - 8) // 2 * ff, ff)]
        return pltpu.make_async_copy(src, gbuf.at[g_slot(m)], gsem.at[g_slot(m)])

    def uk_copy():
        return pltpu.make_async_copy(wuk_ref, gbuf.at[2, :, pl.ds(W4, latent)], xsem.at[0])

    def uv_copy(i):
        return pltpu.make_async_copy(wuv_ref.at[pl.ds(i * hidden, hidden)], gbuf.at[3, :, pl.ds(OB + LN * i, LN)], xsem.at[1 + i])

    def dkv_copy(i):
        lo, size = ((0, ff), (ff, OB))[i]
        return pltpu.make_async_copy(wdkv_ref.at[:, pl.ds(lo, size)], gbuf.at[5, pl.ds(i * lat_row, lat_row), pl.ds(0, size)], xsem.at[5 + i])

    def cache_at(i, slot):
        return slot, pl.ds(i % 4 // 2 * lat_row, lat_row), pl.ds(i % 2 * cache_len, cache_len)

    def c_copy(i, seq, slot):
        return pltpu.make_async_copy(cache_ref.at[seq], dbuf.at[cache_at(i, slot)], csem.at[seq])

    def d_place(p):
        if 8 <= p < 16:
            return gbuf, (2 + (p - 8) // 2, pl.ds(0, ff), pl.ds(p % 2 * dw, dw))
        return dbuf, (p % ND, slice(None), slice(None))

    def d_copy(p):
        if p < 16:
            src = ed_ref.at[p % 4, :, pl.ds((p // 4) * dw, dw)]
        else:
            q = p - 16
            src = sd_ref.at[pl.ds((q % 2) * ff, ff), pl.ds((q // 2) * dw, dw)]
        buf, at = d_place(p)
        return pltpu.make_async_copy(src, buf.at[at], dsem.at[p % 16])

    for k in range(3):
        a_copy(k).start()
    uk_copy().start()
    dkv_copy(0).start()
    dkv_copy(1).start()
    for i in range(num_seq):
        c_copy(i, i, i // 4).start()
    a_copy(3).start()
    for i in range(4):
        uv_copy(i).start()
    a_copy(4).start()

    barrier = pltpu.get_barrier_semaphore()
    peers = [core_peer, y_peer, za_peer, zb_peer]
    for peer in peers:
        pl.semaphore_signal(barrier, inc=1, device_id={"ep": peer}, device_id_type=MESH)

    lane = lax.broadcasted_iota(jnp.int32, (num_seq, LN), 1)
    pad_k = jnp.zeros((8 - top_k, num_seq), F32)
    small = jnp.concatenate([routes_ref[...].astype(F32), pad_k, rgate_ref[...], pad_k, len_ref[...].astype(F32), jnp.zeros((15, num_seq), F32)], axis=0)
    small = jnp.concatenate([small, jnp.zeros((32, LN - num_seq), F32)], axis=1)
    cols = jnp.concatenate([small, jnp.zeros((96, LN), F32)], axis=0).T[:num_seq]
    lenb[...] = jnp.broadcast_to(cols[:, 16:17], (num_seq, LN))
    member = jnp.zeros((num_seq, LN), F32)
    gate_te = jnp.zeros((num_seq, LN), F32)
    for k in range(top_k):
        hit = (lane % 64).astype(F32) == cols[:, k:k + 1]
        member = jnp.where(hit, 1.0, member)
        gate_te = jnp.where(hit, cols[:, 8 + k:9 + k], gate_te)
    tri = jnp.where(lax.broadcasted_iota(jnp.int32, (num_seq, num_seq), 0) > lax.broadcasted_iota(jnp.int32, (num_seq, num_seq), 1), 1.0, 0.0)
    rank = jnp.dot(tri.astype(BF), member.astype(BF), preferred_element_type=F32)
    meta_own[...] = jnp.where(lane < 64, jnp.where(member > 0.5, rank, -4096.0), gate_te)

    freq = jnp.exp((lane % (rope // 2)).astype(F32) * (-2.0 * 9.210340371976184 / rope))
    angle = lenb[...] * freq
    live = lane < rope
    cos_w = jnp.where(live, jnp.cos(angle), 0.0)
    sin_w = jnp.where(live, jnp.where(lane < rope // 2, -jnp.sin(angle), jnp.sin(angle)), 0.0)

    def rotate(v):
        turned = jnp.where(lane < rope // 2, pltpu.roll(v, LN - rope // 2, 1), pltpu.roll(v, rope // 2, 1))
        return v * cos_w + turned * sin_w

    def ag(src_pos, peer, n, own, part_no):
        cc, yy, zz = src_pos
        idx = (cc * 2 + yy) * 4 + zz
        if part_no is None:
            src = meta_own if own else meta_all.at[cc, yy, zz]
            return pltpu.make_async_remote_copy(src_ref=src, dst_ref=meta_all.at[cc, yy, zz], send_sem=am_send.at[n], recv_sem=am_recv.at[idx], device_id={"ep": peer}, device_id_type=MESH)
        cols = pl.ds(part_no * aw, aw)
        src = h_own.at[:, cols] if own else h_all.at[cc, yy, zz, :, cols]
        return pltpu.make_async_remote_copy(src_ref=src, dst_ref=h_all.at[cc, yy, zz, :, cols], send_sem=ag_send.at[part_no * 15 + n], recv_sem=ag_recv.at[part_no * 16 + idx], device_id={"ep": peer}, device_id_type=MESH)

    started = []

    def send(src_pos, peer, n, part_no, own=False):
        a = ag(src_pos, peer, n, own, part_no)
        a.start()
        started.append(a)

    def arrive(src_pos, part_no):
        ag(src_pos, core_peer, 0, False, part_no).wait_recv()

    def send_own(part_no):
        for n, peer in enumerate((zb_peer, y_peer, za_peer, core_peer)):
            send((c, y, z), peer, n, part_no, True)

    def fwd_zb(part_no):
        pos = (c, y, zb)
        arrive(pos, part_no)
        send(pos, za_peer, 4, part_no)
        send(pos, y_peer, 5, part_no)
        send(pos, core_peer, 6, part_no)

    def fwd_za(part_no):
        pos = (c, y, za)
        arrive(pos, part_no)
        send(pos, y_peer, 7, part_no)
        send(pos, core_peer, 8, part_no)

    def fwd_zc(part_no):
        pos = (c, y, zc)
        arrive(pos, part_no)
        send(pos, y_peer, 9, part_no)
        send(pos, core_peer, 10, part_no)

    def fwd_y(i, part_no):
        pos = (c, 1 - y, (z, zb, za, zc)[i])
        arrive(pos, part_no)
        send(pos, core_peer, 11 + i, part_no)

    def hidx(h):
        return h // 8, h // 4 % 2, h % 4

    def q_heads(k, first, count):
        a_copy(k).wait()
        qq = jnp.dot(x_ref[...], gbuf[k, :, pl.ds(0, count * qw)], preferred_element_type=F32).astype(BF).astype(F32)
        for i in range(count // 2):
            pair = qq[:, 2 * i * qw:2 * (i + 1) * qw]
            for h, v in ((first + 2 * i, pair), (first + 2 * i + 1, pltpu.roll(pair, qw, 1))):
                qn[h] = v[:, :nope].astype(BF)
                part[(*hidx(h), slice(None), pl.ds(latent, LN))] = rotate(v[:, nope:nope + LN])

    q_heads(0, 0, 6)
    g_copy(0).start()
    q_heads(1, 6, 6)
    g_copy(1).start()
    q_heads(2, 12, 4)
    uk_copy().wait()
    for h in range(num_heads):
        part[(*hidx(h), slice(None), pl.ds(0, latent))] = jnp.dot(qn[h], gbuf[2, pl.ds(h * nope, nope), pl.ds(W4, latent)], preferred_element_type=F32)
    g_copy(2).start()
    pl.semaphore_wait(barrier, len(peers))
    send_own(None)
    meta_all[c, y, z] = meta_own[...]

    nt = (((1,), (1,)), ((), ()))
    dkv_copy(0).wait()
    dkv_copy(1).wait()
    r = lax.dot_general(x_ref[:, :ff], gbuf[5, pl.ds(0, lat_row), :], nt, preferred_element_type=F32) + lax.dot_general(x_ref[:, ff:], gbuf[5, pl.ds(lat_row, lat_row), pl.ds(0, OB)], nt, preferred_element_type=F32)
    g_copy(5).start()
    r_lat = r[:, :latent].astype(BF)
    r_rope = rotate(jnp.concatenate([r[:, latent:], jnp.zeros((num_seq, LN - rope), F32)], axis=1)).astype(BF)
    kvf[:, :latent] = r_lat.astype(F32)
    kvf[:, latent:] = r_rope.astype(F32)
    kv_ref[:, :latent] = r_lat
    kv_ref[:, latent:] = r_rope[:, :rope]

    scale = qw ** -0.5

    @pl.loop(0, num_seq // 8)
    def _(g):
        for b in range(8):
            c_copy(b, g * 8 + b, 2 * g + b // 4).wait()
        rows8 = pl.ds(pl.multiple_of(g * 8, 8), 8)
        q = part[:, :, :, rows8, pl.ds(0, latent + LN)].reshape(LN, latent + LN).astype(BF)
        kv_rep = jnp.broadcast_to(kvf[rows8, :][None], (16, 8, latent + LN)).reshape(LN, latent + LN)
        n_rep = jnp.broadcast_to(lenb[rows8, :][None], (16, 8, LN)).reshape(LN, LN)
        n_rep = jnp.concatenate([n_rep, n_rep], axis=1)
        row = lax.broadcasted_iota(jnp.int32, (LN, 256), 0) % 8
        pos = lax.broadcasted_iota(jnp.int32, (LN, 256), 1).astype(F32)
        s_new = jnp.sum(q.astype(F32) * kv_rep, axis=1, keepdims=True) * scale
        q = q[:, :latent + rope]
        s = jnp.zeros((LN, 256), F32)
        for b in range(8):
            s = jnp.where(row == b, jnp.dot(q, dbuf[cache_at(b, 2 * g + b // 4)], preferred_element_type=F32), s)
        s = jnp.where(pos < n_rep, s * scale, -jnp.inf)
        top = jnp.maximum(jnp.max(s, axis=1, keepdims=True), s_new)
        e = jnp.exp(s - top)
        e_new = jnp.exp(s_new - top)
        den = jnp.sum(e, axis=1, keepdims=True) + e_new
        p = e / den
        o = (e_new / den).astype(BF).astype(F32) * kv_rep[:, :latent]
        for b in range(8):
            o = o + lax.dot_general(jnp.where(row == b, p, 0.0).astype(BF), dbuf[cache_at(b, 2 * g + b // 4)][:latent], nt, preferred_element_type=F32)
        part[:, :, :, rows8, pl.ds(1024, latent)] = o.reshape(*ZYC, 8, latent)

    for p in range(ND):
        d_copy(p).start()
    fwd_zb(None)
    fwd_za(None)
    for i in range(4):
        uv_copy(i).wait()
    a_copy(3).wait()
    for h in range(num_heads):
        ob = part[(*hidx(h), slice(None), pl.ds(1024, latent))].astype(BF)
        vcat[:, h * LN:(h + 1) * LN] = jnp.dot(ob, gbuf[3, pl.ds(h % 4 * latent, latent), pl.ds(OB + LN * (h // 4), LN)], preferred_element_type=F32).astype(BF)
    a_copy(4).wait()
    fwd_zc(None)
    for lo, hi, slot in ((0, ff, 4), (ff, hidden, 3)):
        a = jnp.dot(vcat[...], gbuf[slot, :, pl.ds(0, hi - lo)], preferred_element_type=F32).astype(BF)
        h_own[:, lo:hi] = (x_ref[:, lo:hi].astype(F32) + a.astype(F32)).astype(BF)
        for i in range(NA):
            if lo < (i + 1) * aw <= hi:
                send_own(i)
    g_copy(3).start()
    g_copy(4).start()
    h_all[c, y, z] = h_own[...]
    for i in range(4):
        fwd_y(i, None)
    fwd_za(0)
    fwd_zb(0)
    fwd_y(0, 0)
    fwd_za(1)
    fwd_zb(1)
    fwd_zc(0)
    fwd_y(0, 1)
    fwd_y(2, 0)
    fwd_y(1, 0)
    fwd_zc(1)

    def gate_up(x, gslot, uslot, store, starts=None):
        for start in starts or range(0, ff, 512):
            size = min(512, ff - start)
            g = jnp.dot(x(), gbuf[gslot, :, pl.ds(start, size)], preferred_element_type=F32)
            u = jnp.dot(x(), gbuf[uslot, :, pl.ds(start, size)], preferred_element_type=F32)
            store(start, size, (g * jax.nn.sigmoid(g) * u).astype(BF))

    def g_wait(k):
        g_copy(k).wait()

    for yy in range(2):
        for zz in range(4):
            arrive((1 - c, yy, zz), None)

    ntok = 16 * num_seq
    rows = 16 * 8
    meta = meta_all[...].reshape(ntok, LN)
    meta_t[...] = meta.T
    lane = lax.broadcasted_iota(jnp.int32, (ntok, LN), 1)
    base_col = lax.broadcasted_iota(jnp.int32, (ntok, LN), 0) // num_seq * 8
    base_row = lax.broadcasted_iota(jnp.int32, (1, ntok), 1) // num_seq * 8
    slot_row = lax.broadcasted_iota(jnp.int32, (rows, ntok), 0)
    for e in range(num_loc):
        ge = me * num_loc + e
        code = jnp.sum(jnp.where(lane == ge, meta, 0.0), axis=1, keepdims=True)
        gate = jnp.sum(jnp.where(lane == ge + 64, meta, 0.0), axis=1, keepdims=True)
        sel[e] = jnp.where(lane == code.astype(jnp.int32) + base_col, 1.0, 0.0).astype(BF)
        gates[e] = jnp.broadcast_to(gate, (ntok, LN))
        code_t = meta_t[pl.ds(ge, 1), :].astype(jnp.int32) + base_row
        sel_t[pl.ds(e * rows, rows), :] = jnp.where(slot_row == code_t, 1.0, 0.0).astype(BF)

    fwd_y(2, 1)
    fwd_y(1, 1)
    fwd_y(3, 0)
    fwd_y(3, 1)
    for i in range(NA):
        for yy in range(2):
            for zz in range(4):
                arrive((1 - c, yy, zz), i)

    @pl.loop(0, hidden // 512)
    def _(n):
        cols = pl.ds(pl.multiple_of(n * 512, 512), 512)
        hh = h_all[:, :, :, :, cols].reshape(ntok, 512)
        xe[:, cols] = jnp.dot(sel_t[...], hh, preferred_element_type=F32).astype(BF)

    for e in range(num_loc):
        g_wait(2 * e)
        g_wait(2 * e + 1)

        def put(start, size, v, e=e):
            act[e, :, pl.ds(start, size)] = v
        gate_up(lambda e=e: xe[pl.ds(e * rows, rows), :], g_slot(2 * e), g_slot(2 * e + 1), put)
        if e == 0:
            g_copy(6).start()
            g_copy(7).start()
        elif e < 3:
            for p in range(4 * e + 4, 4 * e + 8):
                d_copy(p).start()
        else:
            g_copy(8).start()
            g_copy(9).start()

    def rdma(src, dst, send_sem, recv_sem, peer):
        return pltpu.make_async_remote_copy(src_ref=src, dst_ref=dst, send_sem=send_sem, recv_sem=recv_sem, device_id={"ep": peer}, device_id_type=MESH)

    def chunk(j):
        return pl.ds(j * cw, cw)

    def s1(j):
        return rdma(part.at[1 - c, :, :, :, chunk(j)], rc.at[:, :, :, chunk(j)], s1_send.at[j], s1_recv.at[j], core_peer)

    def s2(j):
        return rdma(part.at[c, 1 - y, :, :, chunk(j)], ry.at[:, :, chunk(j)], s2_send.at[j], s2_recv.at[j], y_peer)

    def s3(j, i):
        return rdma(part.at[c, y, (zc, za)[i], :, chunk(j)], rz.at[i, :, chunk(j)], s3_send.at[2 * j + i], s3_recv.at[2 * j + i], za_peer)

    def s4(j):
        return rdma(part.at[c, y, zb, :, chunk(j)], rz.at[2, :, chunk(j)], s4_send.at[j], s4_recv.at[j], zb_peer)

    def step_a(j):
        cols = chunk(j)
        s1(j).wait_recv()
        part[c, 1 - y, :, :, cols] = part[c, 1 - y, :, :, cols] + rc[1 - y, :, :, cols]
        s2(j).start()
        part[c, y, :, :, cols] = part[c, y, :, :, cols] + rc[y, :, :, cols]

    def step_b(j):
        cols = chunk(j)
        s2(j).wait_recv()
        part[c, y, :, :, cols] = part[c, y, :, :, cols] + ry[:, :, cols]
        s3(j, 0).start()
        s3(j, 1).start()

    def step_c(j):
        cols = chunk(j)
        s3(j, 0).wait_recv()
        part[c, y, zb, :, cols] = part[c, y, zb, :, cols] + rz[0, :, cols]
        s4(j).start()

    def t3(j, i):
        return rdma(part.at[c, :, (zc, za)[i], :, chunk(j)], ry.at[pl.ds(2 * i, 2), :, chunk(j)], s3_send.at[2 * j + i], s3_recv.at[2 * j + i], za_peer)

    def t4(j):
        return rdma(part.at[c, :, zb, :, chunk(j)], rz.at[pl.ds(0, 2), :, chunk(j)], s4_send.at[j], s4_recv.at[j], zb_peer)

    def t2(j):
        return rdma(part.at[c, 1 - y, z, :, chunk(j)], rz.at[2, :, chunk(j)], s2_send.at[j], s2_recv.at[j], y_peer)

    def turn_a(j):
        cols = chunk(j)
        s1(j).wait_recv()
        part[c, :, :, :, cols] = part[c, :, :, :, cols] + rc[:, :, :, cols]
        t3(j, 0).start()
        t3(j, 1).start()

    def turn_b(j):
        cols = chunk(j)
        t3(j, 0).wait_recv()
        part[c, :, zb, :, cols] = part[c, :, zb, :, cols] + ry[0:2, :, cols]
        t4(j).start()

    def turn_c(j):
        cols = chunk(j)
        t3(j, 1).wait_recv()
        t4(j).wait_recv()
        part[c, :, z, :, cols] = part[c, :, z, :, cols] + ry[2:4, :, cols] + rz[0:2, :, cols]
        t2(j).start()

    def step_f(j):
        cols = chunk(j)
        if j in YLAST:
            t2(j).wait_recv()
            routed = part[c, y, z, :, cols] + rz[2, :, cols]
        else:
            s3(j, 1).wait_recv()
            s4(j).wait_recv()
            routed = part[c, y, z, :, cols] + rz[1, :, cols] + rz[2, :, cols]
        out_ref[:, cols] = (h_own[:, cols].astype(F32) + shared[:, cols].astype(F32) + routed).astype(BF)

    def down(j):
        cols = chunk(j)
        if j % 2 == 0:
            for e in range(num_loc):
                d_copy(2 * j + e).wait()
        for e in range(num_loc):
            buf, at = d_place(j // 2 * 4 + e)
            o = jnp.dot(act[e], buf[at[0], at[1], pl.ds(j % 2 * cw + (j // 2 > 1) * (e % 2) * dw, cw)] if buf is gbuf else buf[at[0], :, pl.ds(j % 2 * cw, cw)], preferred_element_type=F32).astype(BF)
            b = jnp.dot(sel[e], o, preferred_element_type=F32)
            gt = gates[e]
            b = (b * jnp.concatenate([gt] * (cw // LN), axis=1)).reshape(*ZYC, num_seq, cw)
            if e == 0:
                part[:, :, :, :, cols] = b
            else:
                part[:, :, :, :, cols] = part[:, :, :, :, cols] + b
        if j in (1, 3):
            for e in range(num_loc):
                d_copy(16 + 2 * (j - 1) + e).start()
        if j == 5:
            g_copy(10).start()
            g_copy(11).start()

    def shared_up(i):
        s, b = i // 3, i % 3
        if b == 0:
            g_wait(8 + 2 * s)
            g_wait(9 + 2 * s)

        def put(start, size, v):
            act_sh[s, :, pl.ds(start, size)] = v
        gate_up(lambda: h_own[...], g_slot(8 + 2 * s), g_slot(9 + 2 * s), put, (512 * b,))

    def shared_down(i):
        d_copy(16 + 2 * i).wait()
        d_copy(17 + 2 * i).wait()
        o = jnp.dot(act_sh[0], dbuf[2 * i], preferred_element_type=F32) + jnp.dot(act_sh[1], dbuf[2 * i + 1], preferred_element_type=F32)
        shared[:, i * dw:(i + 1) * dw] = o.astype(BF)

    fill = [lambda i=i: shared_up(i) for i in range(6)] + [lambda i=i: shared_down(i) for i in range(4)]

    def work(n):
        for _ in range(n):
            fill.pop(0)()

    def enter(j):
        (turn_a if j in YLAST else step_a)(j)

    for j in range(NCH):
        down(j)
        s1(j).start()
        if j >= 1:
            enter(j - 1)
        if j == 4:
            turn_b(0)
        if j == 6:
            turn_b(1)
        if j == 7:
            step_b(2)
    enter(7)
    step_b(3)
    step_c(2)
    work(1)
    turn_c(0)
    step_b(4)
    step_c(3)
    work(1)
    turn_c(1)
    step_b(5)
    step_c(4)
    work(1)
    step_b(6)
    step_c(5)
    work(1)
    step_b(7)
    step_c(6)
    work(3)
    step_c(7)
    work(3)
    for j in range(NCH):
        step_f(j)
    for a in started:
        a.wait_send()
    for j in range(NCH):
        s1(j).wait_send()
        if j in YLAST:
            copies = (t2(j), t3(j, 0), t3(j, 1), t4(j))
        else:
            copies = (s2(j), s3(j, 0), s3(j, 1), s4(j))
        for a in copies:
            a.wait_send()


def layer(x, lens, routes, route_gates, cache, w_q, w_dkv, w_uk, w_uv, w_o, sh_gate, sh_up, sh_down, ex_gate, ex_up, ex_down):
    num_seq, hidden = x.shape
    num_loc, _, ff = ex_gate.shape
    lat_row = cache.shape[1]
    ntok = 16 * num_seq
    dma = pltpu.SemaphoreType.DMA
    vm = pl.BlockSpec(memory_space=pltpu.VMEM)
    hbm = pl.BlockSpec(memory_space=pl.ANY)
    return pl.pallas_call(
        layer_kernel,
        out_shape=(jax.ShapeDtypeStruct((num_seq, hidden), BF), jax.ShapeDtypeStruct((num_seq, lat_row), BF)),
        in_specs=[vm] * 4 + [hbm] * 12,
        out_specs=(vm, vm),
        scratch_shapes=[
            pltpu.VMEM((NG, hidden, ff), BF),
            pltpu.VMEM((ND, ff, 2 * hidden // NCH), BF),
            pltpu.VMEM((16, num_seq, LN), BF),
            pltpu.VMEM((num_seq, 640), F32),
            pltpu.VMEM((num_seq, LN), F32),
            pltpu.VMEM((num_seq, hidden), BF),
            pltpu.VMEM((num_seq, hidden), BF),
            pltpu.VMEM((num_seq, LN), F32),
            pltpu.VMEM((*ZYC, num_seq, hidden), BF),
            pltpu.VMEM((*ZYC, num_seq, LN), F32),
            pltpu.VMEM((LN, ntok), F32),
            pltpu.VMEM((num_loc, ntok, LN), BF),
            pltpu.VMEM((num_loc * LN, ntok), BF),
            pltpu.VMEM((num_loc, ntok, LN), F32),
            pltpu.VMEM((num_loc * LN, hidden), BF),
            pltpu.VMEM((num_loc, LN, ff), BF),
            pltpu.VMEM((2, num_seq, ff), BF),
            pltpu.VMEM((num_seq, hidden), BF),
            pltpu.VMEM((*ZYC, num_seq, hidden), F32),
            pltpu.VMEM((2, 4, num_seq, hidden), F32),
            pltpu.VMEM((4, num_seq, hidden), F32),
            pltpu.VMEM((3, num_seq, hidden), F32),
            dma((NG,)), dma((16,)), dma((num_seq,)), dma((7,)), dma((15 * NA,)), dma((16 * NA,)), dma((15,)), dma((16,)),
            dma((NCH,)), dma((NCH,)), dma((NCH,)), dma((NCH,)), dma((2 * NCH,)), dma((2 * NCH,)), dma((NCH,)), dma((NCH,)),
        ],
        compiler_params=pltpu.CompilerParams(collective_id=0, has_side_effects=True, vmem_limit_bytes=67043328),
        name="layer",
    )(x, lens, routes, route_gates, cache, w_q, w_dkv, w_uk, w_uv, w_o, sh_gate, sh_up, sh_down, ex_gate, ex_up, ex_down)


def finish_kernel(a_ref, b_ref, c_ref, d_ref):
    c_ref[...] = a_ref[...]
    d_ref[...] = b_ref[...]


def finish(a, b):
    vm = pl.BlockSpec(memory_space=pltpu.VMEM)
    return pl.pallas_call(finish_kernel, out_shape=(jax.ShapeDtypeStruct(a.shape, a.dtype), jax.ShapeDtypeStruct(b.shape, b.dtype)), in_specs=[vm, vm], out_specs=(vm, vm), name="finish")(a, b)


def solution(mesh):
    def device_step(x_blk, cache_blk, len_blk, routes, route_gates, w_q, w_dkv, w_uk, w_uv, w_o, sh_gate, sh_up, sh_down, ex_gate, ex_up, ex_down):
        lens = len_blk[None, :]
        uk = w_uk.reshape(-1, w_uk.shape[2])
        uv = w_uv.reshape(-1, w_uv.shape[2])
        return finish(*layer(x_blk, lens, routes.T, route_gates.T, cache_blk.transpose(0, 2, 1), w_q, w_dkv.T, uk, uv, w_o, sh_gate, sh_up, sh_down, ex_gate, ex_up, ex_down))

    batch_spec = P(("dp", "ep"))
    weight_spec = P()
    expert_spec = P("ep")
    in_specs = (batch_spec,) * 5 + (weight_spec,) * 8 + (expert_spec,) * 3
    return jax.shard_map(device_step, mesh=mesh, in_specs=in_specs, out_specs=(batch_spec, batch_spec), check_vma=False)
```
